32 devices in a mesh: blk: 8 (over y, x, core), rep: 4 (over z).
Axes of the slice: x: 2, y: 2, z: 4, core: 2. Of those that a mesh axis runs over, the one named last changes fastest.
Arguments:
- image: bfloat16 [4096, 1024], P(('blk', 'rep')), may hold values from -100 to 100
- text: bfloat16 [4096, 1024], P(('blk', 'rep')), may hold values from -100 to 100
- positive: int32 [8, 512], P('blk', 'rep'), may hold values from 0 to 511, each once within a row
- logit_scale: float32 [1], replicated, may hold values from 85 to 270
Outputs:
- row_loss: float32 [4096], P(('blk', 'rep'))
- col_loss: float32 [4096], P(('blk', 'rep'))
- img_grad: float32 [4096, 1024], P(('blk', 'rep'))
- txt_grad: float32 [4096, 1024], P(('blk', 'rep'))
The draws below stay inside these ranges and needn't reach their ends.
Inputs may be any that keep to these rules, and one draw needn't show every extreme that they name: Each row of positive names every index of its block once.
All inputs are finite; a program needn't handle non-finite values.
Results may differ from the reference program's by a relative error of at most 0.0081.
The reference program's roundings to bfloat16 on the way count: a program that leaves them out, or rounds other values in their place, can miss the bound.
Values may be sent and summed in bfloat16 or wider, within the bound.
No kernel may reach another device: no remote copies, remote signals or barrier semaphores. Data moves between devices by JAX's collectives and lax.ppermute only.
A program may use at most 64 MiB of HBM per device.

```python
import jax
import jax.numpy as jnp
from jax import lax

D = 1024
STEPS = 4
BLOCK = 512
BLOCKS = 8
PAIRS = 4096


def embed_pair(key):
    base = jax.random.fold_in(key, 7771)
    key_img, key_txt = jax.random.split(base, 2)
    image = jax.random.truncated_normal(key_img, -6.0, 6.0, (PAIRS, D), jnp.float32)
    text = jax.random.truncated_normal(key_txt, -6.0, 6.0, (PAIRS, D), jnp.float32)
    return (image, text)


def draw_image(key, part):
    return embed_pair(key)[0].astype(jnp.bfloat16)


def draw_text(key, part):
    return embed_pair(key)[1].astype(jnp.bfloat16)


def draw_logit_scale(key, part):
    inner = jax.random.fold_in(key, 55)
    return jax.random.uniform(inner, (1,), jnp.float32, 85.0, 100.0)


def setup_inputs(seed: int = 0) -> dict:
    splits = jax.random.split(jax.random.key(seed), 5)
    image = draw_image(jax.random.fold_in(splits[4], 71), 0)
    text = draw_text(jax.random.fold_in(splits[4], 71), 0)
    positive = jax.vmap(lambda own: jax.random.permutation(own, BLOCK))(jax.random.split(splits[2], BLOCKS)).reshape((BLOCKS, BLOCK)).astype(jnp.int32)
    logit_scale = draw_logit_scale(jax.random.fold_in(splits[4], 71), 0)
    return {"image": image, "text": text, "positive": positive, "logit_scale": logit_scale}


exact_mode = lax.Precision.HIGHEST

def normalize(values):
    widened = values.astype(jnp.float32)
    inverse = lax.rsqrt(lax.optimization_barrier(jnp.sum(widened * widened, axis=-1, keepdims=True)) + 1e-06)
    return (widened * inverse, inverse)

def merge_stats(earlier, later):
    highest = jnp.maximum(earlier[0], later[0])
    summed = earlier[1] * jnp.exp(earlier[0] - highest) + later[1] * jnp.exp(later[0] - highest)
    return (highest, summed)

def reference(image, text, positive, logit_scale):
    factor = logit_scale[0]
    img_unit, img_inverse = normalize(image)
    txt_unit, txt_inverse = normalize(text)
    img_round = lax.optimization_barrier(img_unit.astype(jnp.bfloat16))
    txt_round = lax.optimization_barrier(txt_unit.astype(jnp.bfloat16))
    img_tiles = img_round.astype(jnp.float32).reshape(BLOCKS, BLOCK, D)
    txt_tiles = txt_round.astype(jnp.float32).reshape(BLOCKS, BLOCK, D)
    columns = jnp.arange(BLOCK, dtype=jnp.int32)
    onehot = (positive[:, :, None] == columns[None, None, :]).astype(jnp.float32)

    def scores_at(offset):
        moved = jnp.roll(txt_tiles, offset, axis=0)
        return (moved, factor * jnp.einsum('bid,bjd->bij', img_tiles, moved, precision=exact_mode))
    for offset in range(STEPS):
        moved, scores = scores_at(offset)
        row_peak = lax.optimization_barrier(jnp.max(scores, axis=2))
        col_peak = lax.optimization_barrier(jnp.max(scores, axis=1))
        col_part = lax.optimization_barrier(jnp.sum(jnp.exp(scores - col_peak[:, None, :]), axis=1))
        col_peak = jnp.roll(col_peak, -offset, axis=0)
        col_part = jnp.roll(col_part, -offset, axis=0)
        if offset == 0:
            row_max = row_peak
            row_sum = lax.optimization_barrier(jnp.sum(jnp.exp(scores - row_peak[:, :, None]), axis=2))
            row_pos = lax.optimization_barrier(jnp.sum(onehot * scores, axis=2))
            col_pos = lax.optimization_barrier(jnp.sum(onehot * scores, axis=1))
            col_max, col_sum = (col_peak, col_part)
        else:
            highest = jnp.maximum(row_max, row_peak)
            row_sum = row_sum * jnp.exp(row_max - highest) + lax.optimization_barrier(jnp.sum(jnp.exp(scores - highest[:, :, None]), axis=2))
            row_max = highest
            col_max, col_sum = merge_stats((col_max, col_sum), (col_peak, col_part))
    row_lse = row_max + jnp.log(row_sum)
    col_lse = col_max + jnp.log(col_sum)
    img_sum = jnp.zeros((BLOCKS, BLOCK, D), jnp.float32)
    txt_sum = jnp.zeros((BLOCKS, BLOCK, D), jnp.float32)
    for offset in range(STEPS):
        moved, scores = scores_at(offset)
        col_here = jnp.roll(col_lse, offset, axis=0)
        weight = 0.5 * (jnp.exp(scores - row_lse[:, :, None]) + jnp.exp(scores - col_here[:, None, :]))
        if offset == 0:
            weight = weight - onehot
        weight = lax.optimization_barrier(weight.astype(jnp.bfloat16)).astype(jnp.float32)
        img_sum = img_sum + jnp.einsum('bij,bjd->bid', weight, moved, precision=exact_mode)
        txt_terms = jnp.einsum('bij,bid->bjd', weight, img_tiles, precision=exact_mode)
        txt_sum = txt_sum + jnp.roll(txt_terms, -offset, axis=0)
    img_sum = factor * img_sum.reshape(PAIRS, D)
    txt_sum = factor * txt_sum.reshape(PAIRS, D)
    img_grad = (img_sum - img_unit * lax.optimization_barrier(jnp.sum(img_unit * img_sum, axis=-1, keepdims=True))) * img_inverse
    txt_grad = (txt_sum - txt_unit * lax.optimization_barrier(jnp.sum(txt_unit * txt_sum, axis=-1, keepdims=True))) * txt_inverse
    row_loss = (row_lse - row_pos).reshape(PAIRS)
    col_loss = (col_lse - col_pos).reshape(PAIRS)
    return (row_loss, col_loss, img_grad, txt_grad)
```

```python
import functools

import jax
import jax.numpy as jnp
from jax import lax
from jax.experimental import pallas as pl
from jax.experimental.pallas import tpu as pltpu
from jax.sharding import PartitionSpec as P

STEPS = 4
F32 = jnp.float32
BF16 = jnp.bfloat16
VMEM = pltpu.VMEM
SMEM = pltpu.SMEM


def passed_along(array, axis, by):
    count = lax.axis_size(axis)
    return lax.ppermute(array, axis, [(i, (i + by) % count) for i in range(count)])


def inverse_norm(wide):
    return lax.rsqrt(jnp.sum(wide * wide, axis=-1, keepdims=True) + 1e-06)


def unit_tile(raw):
    wide = raw.astype(F32)
    return (wide * inverse_norm(wide)).astype(BF16)


def diagonal(rows):
    return lax.broadcasted_iota(jnp.int32, (rows, rows), 0) == lax.broadcasted_iota(
        jnp.int32, (rows, rows), 1
    )


def to_lanes(column, eye):
    return jnp.sum(jnp.where(eye, column, 0.0), axis=0, keepdims=True)


def to_column(lanes, eye):
    return jnp.sum(jnp.where(eye, lanes, 0.0), axis=1, keepdims=True)


def onehot_of(positive, eye, parts, rows):
    wanted = to_column(positive.astype(F32), eye)
    lane = lax.broadcasted_iota(jnp.int32, (rows, rows), 1)
    quarter = lax.axis_index("rep")
    return [
        wanted == (lane + lax.rem(quarter - s + parts, parts) * rows).astype(F32)
        for s in range(parts)
    ]


def scores_kernel(parts, scale, positive, *refs):
    images, texts = refs[:STEPS], refs[STEPS : STEPS + parts]
    scores, img_out, txt_out, row_stats, col_stats, row_pos = refs[STEPS + parts :]
    rows = images[0].shape[0]
    factor = scale[0]
    eye = diagonal(rows)
    onehot = onehot_of(positive[...], eye, parts, rows)
    for s in range(parts):
        txt_out[s * rows : (s + 1) * rows, :] = unit_tile(texts[s][...])
    for k in range(STEPS):
        img_out[k * rows : (k + 1) * rows, :] = unit_tile(images[k][...])
    scores[...] = factor * lax.dot_general(
        img_out[...], txt_out[...], (((1,), (1,)), ((), ())), preferred_element_type=F32
    )
    peaks, sums = [], []
    for k in range(STEPS):
        tile = scores[k * rows : (k + 1) * rows, :]
        peak = jnp.max(tile, axis=1, keepdims=True)
        peaks.append(to_lanes(peak, eye))
        sums.append(to_lanes(jnp.sum(jnp.exp(tile - peak), axis=1, keepdims=True), eye))
    row_stats[...] = jnp.concatenate(peaks + sums, axis=0)
    peaks, sums, picked = [], [], []
    found = jnp.zeros((rows, 1), F32)
    for s in range(parts):
        tile = scores[:, s * rows : (s + 1) * rows]
        peak = jnp.max(tile, axis=0, keepdims=True)
        peaks.append(peak)
        sums.append(jnp.sum(jnp.exp(tile - peak), axis=0, keepdims=True))
        chosen = jnp.where(onehot[s], tile[:rows, :], 0.0)
        picked.append(jnp.sum(chosen, axis=0, keepdims=True))
        found = found + jnp.sum(chosen, axis=1, keepdims=True)
    row_pos[...] = to_lanes(found, eye)
    col_stats[...] = jnp.concatenate(peaks + sums + picked, axis=0)


def merged(parts):
    peak = functools.reduce(jnp.maximum, [p for p, _ in parts])
    total = sum(s * jnp.exp(p - peak) for p, s in parts)
    return peak + jnp.log(total)


def grads_kernel(parts, positive, scores, images, texts, row_pos, *refs):
    row_stats, col_stats = refs[: 2 * STEPS - 1], refs[2 * STEPS - 1 : 2 * STEPS - 1 + parts]
    outs = refs[2 * STEPS - 1 + parts : -1]
    weights = refs[-1]
    row_loss, col_loss = outs[:2]
    img_parts, txt_parts = outs[2 : 2 + STEPS], outs[2 + STEPS :]
    rows = row_pos.shape[1]
    eye = diagonal(rows)
    onehot = onehot_of(positive[...], eye, parts, rows)

    def row_pair(shift, k):
        table = row_stats[shift + STEPS - 1]
        return table[k + shift : k + shift + 1, :], table[
            STEPS + k + shift : STEPS + k + shift + 1, :
        ]

    row_lse = []
    for k in range(STEPS):
        lse = merged(
            [row_pair(t, k) for t in range(1 - STEPS, STEPS) if 0 <= k + t < STEPS]
        )
        if k == 0:
            row_loss[...] = lse - row_pos[...]
        row_lse.append(to_column(lse, eye))
    col_lse = []
    for s in range(parts):
        at = [(t, (s - t) % parts) for t in range(parts)]
        lse = merged(
            [(col_stats[t][q : q + 1, :], col_stats[t][parts + q : parts + q + 1, :]) for t, q in at]
        )
        if s == 0:
            picked = sum(col_stats[t][2 * parts + q : 2 * parts + q + 1, :] for t, q in at)
            col_loss[...] = lse - picked
        col_lse.append(lse)
    for k in range(STEPS):
        for s in range(parts):
            tile = scores[k * rows : (k + 1) * rows, s * rows : (s + 1) * rows]
            weight = 0.5 * (jnp.exp(tile - row_lse[k]) + jnp.exp(tile - col_lse[s]))
            if k == 0:
                weight = weight - onehot[s].astype(F32)
            weights[k * rows : (k + 1) * rows, s * rows : (s + 1) * rows] = weight.astype(BF16)
    for s in range(parts - 1, -1, -1):
        part = lax.dot_general(
            weights[:, s * rows : (s + 1) * rows],
            images[...],
            (((0,), (0,)), ((), ())),
            preferred_element_type=F32,
        )
        txt_parts[s][...] = part.astype(txt_parts[s].dtype)
    for k in range(STEPS):
        part = jnp.dot(
            weights[k * rows : (k + 1) * rows, :], texts[...], preferred_element_type=F32
        )
        img_parts[k][...] = part.astype(img_parts[k].dtype)


def final_kernel(scale, raw, *refs):
    grad = refs[-1]
    wide = raw[...].astype(F32)
    inverse = inverse_norm(wide)
    unit = wide * inverse
    total = scale[0] * sum(part[...].astype(F32) for part in refs[:-1])
    grad[...] = (total - unit * jnp.sum(unit * total, axis=-1, keepdims=True)) * inverse


def call(kernel, outs, specs, args, scratch=(), name=None):
    return pl.pallas_call(
        kernel,
        out_shape=outs,
        in_specs=[pl.BlockSpec(memory_space=space) for space in specs],
        out_specs=jax.tree.map(lambda _: pl.BlockSpec(memory_space=VMEM), outs),
        scratch_shapes=list(scratch),
        name=name,
    )(*args)


def on_device(image, text, positive, logit_scale):
    rows, width = image.shape
    parts = lax.axis_size("rep")
    shape = jax.ShapeDtypeStruct
    texts = [text] + [passed_along(text, "rep", t) for t in range(1, parts)]
    images = [image] + [passed_along(image, "blk", -k) for k in range(1, STEPS)]
    scores, img_tiles, txt_tiles, row_stats, col_stats, row_pos = call(
        functools.partial(scores_kernel, parts),
        (
            shape((STEPS * rows, parts * rows), F32),
            shape((STEPS * rows, width), BF16),
            shape((parts * rows, width), BF16),
            shape((2 * STEPS, rows), F32),
            shape((3 * parts, rows), F32),
            shape((1, rows), F32),
        ),
        [SMEM] + [VMEM] * (1 + STEPS + parts),
        (logit_scale, positive, *images, *texts),
        name="scores",
    )
    col_tables = [col_stats] + [passed_along(col_stats, "rep", t) for t in range(1, parts)]
    row_tables = [
        row_stats if t == 0 else passed_along(row_stats, "blk", t)
        for t in range(1 - STEPS, STEPS)
    ]
    row_loss, col_loss, *partials = call(
        functools.partial(grads_kernel, parts),
        (
            shape((1, rows), F32),
            shape((1, rows), F32),
            *[shape((rows, width), BF16 if k else F32) for k in range(STEPS)],
            *[shape((rows, width), BF16 if s else F32) for s in range(parts)],
        ),
        [VMEM] * (5 + 2 * STEPS - 1 + parts),
        (positive, scores, img_tiles, txt_tiles, row_pos, *row_tables, *col_tables),
        scratch=[pltpu.VMEM((STEPS * rows, parts * rows), BF16)],
        name="grads",
    )
    img_parts, txt_parts = partials[:STEPS], partials[STEPS:]
    txt_sums = [txt_parts[0]] + [
        passed_along(txt_parts[s], "rep", -s) for s in range(1, parts)
    ]
    img_sums = [img_parts[0]] + [passed_along(img_parts[k], "blk", k) for k in range(1, STEPS)]
    grads = [
        call(
            final_kernel,
            shape((rows, width), F32),
            [SMEM] + [VMEM] * (1 + len(sums)),
            (logit_scale, raw, *sums),
            name=name,
        )
        for raw, sums, name in ((image, img_sums, "img_final"), (text, txt_sums, "txt_final"))
    ]
    return (row_loss[0], col_loss[0], *grads)


def solution(mesh):
    placed = (P(("blk", "rep"), None), P(("blk", "rep"), None), P("blk", "rep"), P())
    return jax.shard_map(
        on_device,
        mesh=mesh,
        in_specs=placed,
        out_specs=(
            P(("blk", "rep")),
            P(("blk", "rep")),
            P(("blk", "rep"), None),
            P(("blk", "rep"), None),
        ),
        check_vma=False,
    )
```

```python
import functools

import jax
import jax.numpy as jnp
from jax import lax
from jax.experimental import pallas as pl
from jax.experimental.pallas import tpu as pltpu
from jax.sharding import PartitionSpec as P

STEPS = 4
CHUNK = 16
F32 = jnp.float32
BF16 = jnp.bfloat16
VMEM = pltpu.VMEM
SMEM = pltpu.SMEM


def power_of_two(count):
    return count & (count - 1) == 0


def place(own, slot, count):
    return own ^ slot if power_of_two(count) else (own + slot) % count


def slot_at(slot, partner, count):
    return slot ^ partner if power_of_two(count) else (slot - partner) % count


def fetched(array, axis, slot):
    count = lax.axis_size(axis)
    return lax.ppermute(array, axis, [(place(i, slot, count), i) for i in range(count)])


def returned(array, axis, slot):
    count = lax.axis_size(axis)
    return lax.ppermute(array, axis, [(i, place(i, slot, count)) for i in range(count)])


def passed_along(array, axis, by):
    count = lax.axis_size(axis)
    return lax.ppermute(array, axis, [(i, (i + by) % count) for i in range(count)])


def inverse_norm(wide):
    return lax.rsqrt(jnp.sum(wide * wide, axis=-1, keepdims=True) + 1e-06)


def store_units(raw, out, base):
    for at in range(0, raw.shape[0], CHUNK):
        wide = raw[at : at + CHUNK, :].astype(F32)
        out[base + at : base + at + CHUNK, :] = (wide * inverse_norm(wide)).astype(BF16)


def diagonal(rows):
    return lax.broadcasted_iota(jnp.int32, (rows, rows), 0) == lax.broadcasted_iota(
        jnp.int32, (rows, rows), 1
    )


def to_lanes(column, eye):
    return jnp.sum(jnp.where(eye, column, 0.0), axis=0, keepdims=True)


def to_column(lanes, eye):
    return jnp.sum(jnp.where(eye, lanes, 0.0), axis=1, keepdims=True)


def onehot_of(positive, eye, parts, rows):
    wanted = to_column(positive.astype(F32), eye)
    lane = lax.broadcasted_iota(jnp.int32, (rows, rows), 1)
    quarter = lax.axis_index("rep")
    return [wanted == (lane + place(quarter, s, parts) * rows).astype(F32) for s in range(parts)]


def scores_kernel(parts, scale, positive, *refs):
    images, texts = refs[:STEPS], refs[STEPS : STEPS + parts]
    scores, img_out, txt_out, row_stats, col_stats, row_pos = refs[STEPS + parts :]
    rows = images[0].shape[0]
    factor = scale[0]
    eye = diagonal(rows)
    onehot = onehot_of(positive[...], eye, parts, rows)
    for s in range(parts):
        store_units(texts[s], txt_out, s * rows)
    for k in range(STEPS):
        store_units(images[k], img_out, k * rows)
    scores[...] = factor * lax.dot_general(
        img_out[...], txt_out[...], (((1,), (1,)), ((), ())), preferred_element_type=F32
    )
    peaks, sums = [], []
    for k in range(STEPS):
        tile = scores[k * rows : (k + 1) * rows, :]
        peak = jnp.max(tile, axis=1, keepdims=True)
        peaks.append(to_lanes(peak, eye))
        sums.append(to_lanes(jnp.sum(jnp.exp(tile - peak), axis=1, keepdims=True), eye))
    row_stats[...] = jnp.concatenate(peaks + sums, axis=0)
    peaks, sums, picked = [], [], []
    found = jnp.zeros((rows, 1), F32)
    for s in range(parts):
        tile = scores[:, s * rows : (s + 1) * rows]
        peak = jnp.max(tile, axis=0, keepdims=True)
        peaks.append(peak)
        sums.append(jnp.sum(jnp.exp(tile - peak), axis=0, keepdims=True))
        chosen = jnp.where(onehot[s], tile[:rows, :], 0.0)
        picked.append(jnp.sum(chosen, axis=0, keepdims=True))
        found = found + jnp.sum(chosen, axis=1, keepdims=True)
    row_pos[...] = to_lanes(found, eye)
    col_stats[...] = jnp.concatenate(peaks + sums + picked, axis=0)


def merged(pairs):
    peak = functools.reduce(jnp.maximum, [p for p, _ in pairs])
    return peak + jnp.log(sum(s * jnp.exp(p - peak) for p, s in pairs))


def weights_kernel(parts, positive, scores, images, row_pos, *refs):
    row_stats, col_stats = refs[: 2 * STEPS - 1], refs[2 * STEPS - 1 : 2 * STEPS - 1 + parts]
    row_loss, col_loss, weights, *txt_parts = refs[2 * STEPS - 1 + parts :]
    rows = row_pos.shape[1]
    eye = diagonal(rows)
    onehot = onehot_of(positive[...], eye, parts, rows)

    def row_pair(shift, k):
        table = row_stats[shift + STEPS - 1]
        at = k + shift
        return table[at : at + 1, :], table[STEPS + at : STEPS + at + 1, :]

    row_lse = []
    for k in range(STEPS):
        lse = merged([row_pair(t, k) for t in range(1 - STEPS, STEPS) if 0 <= k + t < STEPS])
        if k == 0:
            row_loss[...] = lse - row_pos[...]
        row_lse.append(to_column(lse, eye))
    col_lse = []
    for s in range(parts):
        at = [(t, slot_at(s, t, parts)) for t in range(parts)]
        lse = merged(
            [(col_stats[t][q : q + 1, :], col_stats[t][parts + q : parts + q + 1, :]) for t, q in at]
        )
        if s == 0:
            picked = sum(col_stats[t][2 * parts + q : 2 * parts + q + 1, :] for t, q in at)
            col_loss[...] = lse - picked
        col_lse.append(lse)
    for s in range(parts):
        for k in range(STEPS):
            tile = scores[k * rows : (k + 1) * rows, s * rows : (s + 1) * rows]
            weight = 0.5 * (jnp.exp(tile - row_lse[k]) + jnp.exp(tile - col_lse[s]))
            if k == 0:
                weight = weight - onehot[s].astype(F32)
            weights[k * rows : (k + 1) * rows, s * rows : (s + 1) * rows] = weight.astype(BF16)
    for s in range(parts):
        part = lax.dot_general(
            weights[:, s * rows : (s + 1) * rows],
            images[...],
            (((0,), (0,)), ((), ())),
            preferred_element_type=F32,
        )
        txt_parts[s][...] = part.astype(txt_parts[s].dtype)


def images_kernel(weights, texts, *img_parts):
    rows = img_parts[0].shape[0]
    for k in range(STEPS):
        part = jnp.dot(
            weights[k * rows : (k + 1) * rows, :], texts[...], preferred_element_type=F32
        )
        img_parts[k][...] = part.astype(img_parts[k].dtype)


def final_kernel(scale, raw, *refs):
    grad = refs[-1]
    factor = scale[0]
    for at in range(0, raw.shape[0], CHUNK):
        chunk = slice(at, at + CHUNK)
        wide = raw[chunk, :].astype(F32)
        inverse = inverse_norm(wide)
        unit = wide * inverse
        total = factor * sum(part[chunk, :].astype(F32) for part in refs[:-1])
        along = jnp.sum(unit * total, axis=-1, keepdims=True)
        grad[chunk, :] = (total - unit * along) * inverse


def call(kernel, outs, specs, args):
    return pl.pallas_call(
        kernel,
        out_shape=outs,
        in_specs=[pl.BlockSpec(memory_space=space) for space in specs],
        out_specs=jax.tree.map(lambda _: pl.BlockSpec(memory_space=VMEM), outs),
        compiler_params=pltpu.CompilerParams(vmem_limit_bytes=16 << 20),
    )(*args)


def on_device(image, text, positive, logit_scale):
    rows, width = image.shape
    parts = lax.axis_size("rep")
    shape = jax.ShapeDtypeStruct
    texts = [text] + [fetched(text, "rep", s) for s in range(1, parts)]
    images = [image] + [passed_along(image, "blk", -k) for k in range(1, STEPS)]
    scores, img_tiles, txt_tiles, row_stats, col_stats, row_pos = call(
        functools.partial(scores_kernel, parts),
        (
            shape((STEPS * rows, parts * rows), F32),
            shape((STEPS * rows, width), BF16),
            shape((parts * rows, width), BF16),
            shape((2 * STEPS, rows), F32),
            shape((3 * parts, rows), F32),
            shape((1, rows), F32),
        ),
        [SMEM] + [VMEM] * (1 + STEPS + parts),
        (logit_scale, positive, *images, *texts),
    )
    col_tables = [col_stats] + [fetched(col_stats, "rep", t) for t in range(1, parts)]
    row_tables = [
        row_stats if t == 0 else passed_along(row_stats, "blk", t)
        for t in range(1 - STEPS, STEPS)
    ]
    row_loss, col_loss, weights, *txt_parts = call(
        functools.partial(weights_kernel, parts),
        (
            shape((1, rows), F32),
            shape((1, rows), F32),
            shape((STEPS * rows, parts * rows), BF16),
            *[shape((rows, width), BF16 if s else F32) for s in range(parts)],
        ),
        [VMEM] * (4 + 2 * STEPS - 1 + parts),
        (positive, scores, img_tiles, row_pos, *row_tables, *col_tables),
    )
    txt_sums = [txt_parts[0]] + [returned(txt_parts[s], "rep", s) for s in range(1, parts)]
    img_parts = call(
        images_kernel,
        [shape((rows, width), BF16 if k else F32) for k in range(STEPS)],
        [VMEM] * 2,
        (weights, txt_tiles),
    )
    img_sums = [img_parts[0]] + [passed_along(img_parts[k], "blk", k) for k in range(1, STEPS)]
    grads = [
        call(
            final_kernel,
            shape((rows, width), F32),
            [SMEM] + [VMEM] * (1 + len(sums)),
            (logit_scale, raw, *sums),
        )
        for raw, sums in ((image, img_sums), (text, txt_sums))
    ]
    return (row_loss[0], col_loss[0], *grads)


def solution(mesh):
    placed = (P(("blk", "rep"), None), P(("blk", "rep"), None), P("blk", "rep"), P())

    return jax.shard_map(
        on_device,
        mesh=mesh,
        in_specs=placed,
        out_specs=(
            P(("blk", "rep")),
            P(("blk", "rep")),
            P(("blk", "rep"), None),
            P(("blk", "rep"), None),
        ),
        check_vma=False,
    )
```

```python
import functools

import jax
import jax.numpy as jnp
from jax import lax
from jax.experimental import pallas as pl
from jax.experimental.pallas import tpu as pltpu
from jax.sharding import PartitionSpec as P

STEPS = 4
CHUNK = 16
F32 = jnp.float32
BF16 = jnp.bfloat16
VMEM = pltpu.VMEM
SMEM = pltpu.SMEM


def power_of_two(count):
    return count & (count - 1) == 0


def place(own, slot, count):
    return own ^ slot if power_of_two(count) else (own + slot) % count


def slot_at(slot, partner, count):
    return slot ^ partner if power_of_two(count) else (slot - partner) % count


def fetched(array, axis, slot):
    count = lax.axis_size(axis)
    return lax.ppermute(array, axis, [(place(i, slot, count), i) for i in range(count)])


def returned(array, axis, slot):
    count = lax.axis_size(axis)
    return lax.ppermute(array, axis, [(i, place(i, slot, count)) for i in range(count)])


def passed_along(array, axis, by):
    count = lax.axis_size(axis)
    return lax.ppermute(array, axis, [(i, (i + by) % count) for i in range(count)])


def table_rows(parts):
    return -(-3 * parts // 8) * 8


def doublings(reach):
    known, rounds = 0, []
    while known < reach:
        shift = min(2 * known + 1, reach - known)
        rounds.append((shift, known))
        known += shift
    return rounds


def known_places(reach):
    held = [[0]]
    for shift, known in doublings(reach):
        for centre in (shift, -shift):
            held.append(list(range(centre - known, centre + known + 1)))
    return held


def slot_counts(parts):
    counts = [1]
    while sum(counts) < parts:
        counts.append(min(sum(counts), parts - sum(counts)))
    return counts


def inverse_norm(wide):
    return lax.rsqrt(jnp.sum(wide * wide, axis=-1, keepdims=True) + 1e-06)


def store_units(raw, out, base):
    for at in range(0, raw.shape[0], CHUNK):
        wide = raw[at : at + CHUNK, :].astype(F32)
        out[base + at : base + at + CHUNK, :] = (wide * inverse_norm(wide)).astype(BF16)


def diagonal(rows):
    return lax.broadcasted_iota(jnp.int32, (rows, rows), 0) == lax.broadcasted_iota(
        jnp.int32, (rows, rows), 1
    )


def to_lanes(column, eye):
    return jnp.sum(jnp.where(eye, column, 0.0), axis=0, keepdims=True)


def to_column(lanes, eye):
    return jnp.sum(jnp.where(eye, lanes, 0.0), axis=1, keepdims=True)


def onehot_of(positive, eye, parts, rows):
    wanted = to_column(positive.astype(F32), eye)
    lane = lax.broadcasted_iota(jnp.int32, (rows, rows), 1)
    quarter = lax.axis_index("rep")
    return [wanted == (lane + place(quarter, s, parts) * rows).astype(F32) for s in range(parts)]


def scores_kernel(parts, slots, factor, positive, images, texts, scores, txt_out, row_out, col_out):
    rows = texts[0].shape[0]
    eye = diagonal(rows)
    wanted = to_column(positive.astype(F32), eye)
    lane = lax.broadcasted_iota(jnp.int32, (rows, rows), 1)
    quarter = lax.axis_index("rep")
    for n, text in enumerate(texts):
        store_units(text, txt_out, n * rows)
    scores[...] = factor * lax.dot_general(
        images[...], txt_out[...], (((1,), (1,)), ((), ())), preferred_element_type=F32
    )
    peaks, sums = [], []
    for k in range(STEPS):
        tile = scores[k * rows : (k + 1) * rows, :]
        peak = jnp.max(tile, axis=1, keepdims=True)
        peaks.append(to_lanes(peak, eye))
        sums.append(to_lanes(jnp.sum(jnp.exp(tile - peak), axis=1, keepdims=True), eye))
    found = jnp.zeros((rows, 1), F32)
    col_peaks, col_sums, picked = [], [], []
    for n, s in enumerate(slots):
        tile = scores[:, n * rows : (n + 1) * rows]
        peak = jnp.max(tile, axis=0, keepdims=True)
        col_peaks.append(peak)
        col_sums.append(jnp.sum(jnp.exp(tile - peak), axis=0, keepdims=True))
        match = wanted == (lane + place(quarter, s, parts) * rows).astype(F32)
        chosen = jnp.where(match, tile[:rows, :], 0.0)
        picked.append(jnp.sum(chosen, axis=0, keepdims=True))
        found = found + jnp.sum(chosen, axis=1, keepdims=True)
    row_out[...] = jnp.concatenate(peaks + sums + [to_lanes(found, eye)], axis=0)
    col_out[...] = jnp.concatenate(col_peaks + col_sums + picked, axis=0)


def first_kernel(parts, scale, positive, *refs):
    images, texts = refs[:STEPS], refs[STEPS : STEPS + parts - 1]
    img_out, *outs = refs[STEPS + parts - 1 :]
    rows = images[0].shape[0]
    for k in range(STEPS):
        store_units(images[k], img_out, k * rows)
    slots = range(parts - 1)
    scores_kernel(parts, slots, scale[0], positive[...], img_out, texts, *outs)


def last_kernel(parts, scale, positive, images, text, row_first, col_first, *outs):
    *outs, row_stats, col_stats, row_pos, row_last, col_last = outs
    slots = [parts - 1]
    scores_kernel(
        parts, slots, scale[0], positive[...], images, [text], *outs, row_last, col_last
    )
    peaks = jnp.maximum(row_first[:STEPS, :], row_last[:STEPS, :])
    sums = sum(
        t[STEPS : 2 * STEPS, :] * jnp.exp(t[:STEPS, :] - peaks) for t in (row_first, row_last)
    )
    row_stats[...] = jnp.concatenate([peaks, sums], axis=0)
    row_pos[...] = row_first[2 * STEPS :, :] + row_last[2 * STEPS :, :]
    tables = []
    for which in range(3):
        tables += [col_first[which * (parts - 1) : (which + 1) * (parts - 1), :]]
        tables += [col_last[which : which + 1, :]]
    blank = jnp.zeros((col_stats.shape[0] - 3 * parts, col_last.shape[1]), F32)
    col_stats[...] = jnp.concatenate(tables + [blank] * (blank.shape[0] > 0), axis=0)


def merged(pairs):
    peak = functools.reduce(jnp.maximum, [p for p, _ in pairs])
    return peak + jnp.log(sum(s * jnp.exp(p - peak) for p, s in pairs))


def weights_kernel(parts, positive, first, last, images, row_pos, *refs):
    places = known_places(STEPS - 1)
    row_refs, refs = refs[: len(places)], refs[len(places) :]
    held = slot_counts(parts)
    col_refs, refs = refs[: len(held)], refs[len(held) :]
    row_loss, col_loss, weights, *txt_parts = refs
    rows = row_pos.shape[1]
    eye = diagonal(rows)
    onehot = onehot_of(positive[...], eye, parts, rows)
    row_tables = {}
    for ref, shifts in zip(row_refs, places):
        for n, shift in enumerate(shifts):
            row_tables[shift] = ref[n * 2 * STEPS : (n + 1) * 2 * STEPS, :]
    height = table_rows(parts)
    col_tables = []
    for ref, count in zip(col_refs, held):
        col_tables += [ref[n * height : (n + 1) * height, :] for n in range(count)]

    def row_pair(shift, k):
        table, at = row_tables[shift], k - shift
        return table[at : at + 1, :], table[STEPS + at : STEPS + at + 1, :]

    row_lse = []
    for k in range(STEPS):
        lse = merged([row_pair(t, k) for t in range(1 - STEPS, STEPS) if 0 <= k - t < STEPS])
        if k == 0:
            row_loss[...] = lse - row_pos[...]
        row_lse.append(to_column(lse, eye))
    col_lse = []
    for s in range(parts):
        at = [(col_tables[t], slot_at(s, t, parts)) for t in range(parts)]
        lse = merged([(c[q : q + 1, :], c[parts + q : parts + q + 1, :]) for c, q in at])
        if s == 0:
            col_loss[...] = lse - sum(c[2 * parts + q : 2 * parts + q + 1, :] for c, q in at)
        col_lse.append(lse)
    for s in range(parts):
        source, base = (first, s * rows) if s < parts - 1 else (last, 0)
        for k in range(STEPS):
            tile = source[k * rows : (k + 1) * rows, base : base + rows]
            weight = 0.5 * (jnp.exp(tile - row_lse[k]) + jnp.exp(tile - col_lse[s]))
            if k == 0:
                weight = weight - onehot[s].astype(F32)
            weights[k * rows : (k + 1) * rows, s * rows : (s + 1) * rows] = weight.astype(BF16)
    for s in range(parts):
        part = lax.dot_general(
            weights[:, s * rows : (s + 1) * rows],
            images[...],
            (((0,), (0,)), ((), ())),
            preferred_element_type=F32,
        )
        txt_parts[s][...] = part.astype(txt_parts[s].dtype)


def images_kernel(weights, first, last, *img_parts):
    rows = img_parts[0].shape[0]
    split = first.shape[0]
    for k in range(STEPS):
        strip = slice(k * rows, (k + 1) * rows)
        part = jnp.dot(weights[strip, :split], first[...], preferred_element_type=F32)
        part = part + jnp.dot(weights[strip, split:], last[...], preferred_element_type=F32)
        img_parts[k][...] = part.astype(img_parts[k].dtype)


def final_kernel(scale, raw, *refs):
    grad = refs[-1]
    factor = scale[0]
    for at in range(0, raw.shape[0], CHUNK):
        chunk = slice(at, at + CHUNK)
        wide = raw[chunk, :].astype(F32)
        inverse = inverse_norm(wide)
        unit = wide * inverse
        total = factor * sum(part[chunk, :].astype(F32) for part in refs[:-1])
        along = jnp.sum(unit * total, axis=-1, keepdims=True)
        grad[chunk, :] = (total - unit * along) * inverse


def call(kernel, outs, specs, args, scratch=()):
    return pl.pallas_call(
        kernel,
        out_shape=outs,
        in_specs=[pl.BlockSpec(memory_space=space) for space in specs],
        out_specs=jax.tree.map(lambda _: pl.BlockSpec(memory_space=VMEM), outs),
        scratch_shapes=list(scratch),
        compiler_params=pltpu.CompilerParams(vmem_limit_bytes=16 << 20),
    )(*args)


def on_device(image, text, positive, logit_scale):
    rows, width = image.shape
    parts = lax.axis_size("rep")
    height = table_rows(parts)
    shape = jax.ShapeDtypeStruct
    texts = [text] + [fetched(text, "rep", s) for s in range(1, parts)]
    images = [image] + [passed_along(image, "blk", -k) for k in range(1, STEPS)]
    split = (parts - 1) * rows
    img_tiles, first, txt_first, row_first, col_first = call(
        functools.partial(first_kernel, parts),
        (
            shape((STEPS * rows, width), BF16),
            shape((STEPS * rows, split), F32),
            shape((split, width), BF16),
            shape((2 * STEPS + 1, rows), F32),
            shape((3 * (parts - 1), rows), F32),
        ),
        [SMEM] + [VMEM] * (STEPS + parts),
        (logit_scale, positive, *images, *texts[:-1]),
    )
    last, txt_last, row_stats, col_stats, row_pos = call(
        functools.partial(last_kernel, parts),
        (
            shape((STEPS * rows, rows), F32),
            shape((rows, width), BF16),
            shape((2 * STEPS, rows), F32),
            shape((height, rows), F32),
            shape((1, rows), F32),
        ),
        [SMEM] + [VMEM] * 5,
        (logit_scale, positive, img_tiles, texts[-1], row_first, col_first),
        [pltpu.VMEM((2 * STEPS + 1, rows), F32), pltpu.VMEM((3, rows), F32)],
    )
    col_tables = [col_stats]
    for n, count in enumerate(slot_counts(parts)[1:]):
        sent = jnp.concatenate(col_tables, axis=0)[: count * height]
        col_tables.append(fetched(sent, "rep", 2**n))
    row_tables = [row_stats]
    for shift, known in doublings(STEPS - 1):
        by_shift = {}
        for array, shifts in zip(row_tables, known_places(STEPS - 1)):
            for at, place_ in enumerate(shifts):
                by_shift[place_] = array[at * 2 * STEPS : (at + 1) * 2 * STEPS]
        sent = jnp.concatenate([by_shift[t] for t in range(-known, known + 1)], axis=0)
        for sign in (1, -1):
            row_tables.append(passed_along(sent, "blk", -sign * shift))
    row_loss, col_loss, weights, *txt_parts = call(
        functools.partial(weights_kernel, parts),
        (
            shape((1, rows), F32),
            shape((1, rows), F32),
            shape((STEPS * rows, parts * rows), BF16),
            *[shape((rows, width), BF16 if s else F32) for s in range(parts)],
        ),
        [VMEM] * (5 + len(row_tables) + len(col_tables)),
        (positive, first, last, img_tiles, row_pos, *row_tables, *col_tables),
    )
    txt_sums = [txt_parts[0]] + [returned(txt_parts[s], "rep", s) for s in range(1, parts)]
    img_parts = call(
        images_kernel,
        [shape((rows, width), BF16 if k else F32) for k in range(STEPS)],
        [VMEM] * 3,
        (weights, txt_first, txt_last),
    )
    img_sums = [img_parts[0]] + [passed_along(img_parts[k], "blk", k) for k in range(1, STEPS)]
    grads = [
        call(
            final_kernel,
            shape((rows, width), F32),
            [SMEM] + [VMEM] * (1 + len(sums)),
            (logit_scale, raw, *sums),
        )
        for raw, sums in ((image, img_sums), (text, txt_sums))
    ]
    return (row_loss[0], col_loss[0], *grads)


def solution(mesh):
    placed = (P(("blk", "rep"), None), P(("blk", "rep"), None), P("blk", "rep"), P())

    return jax.shard_map(
        on_device,
        mesh=mesh,
        in_specs=placed,
        out_specs=(
            P(("blk", "rep")),
            P(("blk", "rep")),
            P(("blk", "rep"), None),
            P(("blk", "rep"), None),
        ),
        check_vma=False,
    )
```

```python
import functools

import jax
import jax.numpy as jnp
from jax import lax
from jax.experimental import pallas as pl
from jax.experimental.pallas import tpu as pltpu
from jax.sharding import PartitionSpec as P

STEPS = 4
CHUNK = 16
F32 = jnp.float32
BF16 = jnp.bfloat16
VMEM = pltpu.VMEM
SMEM = pltpu.SMEM


def power_of_two(count):
    return count & (count - 1) == 0


def place(own, slot, count):
    return own ^ slot if power_of_two(count) else (own + slot) % count


def slot_at(slot, partner, count):
    return slot ^ partner if power_of_two(count) else (slot - partner) % count


def fetched(array, axis, slot):
    count = lax.axis_size(axis)
    return lax.ppermute(array, axis, [(place(i, slot, count), i) for i in range(count)])


def returned(array, axis, slot):
    count = lax.axis_size(axis)
    return lax.ppermute(array, axis, [(i, place(i, slot, count)) for i in range(count)])


def passed_along(array, axis, by):
    count = lax.axis_size(axis)
    return lax.ppermute(array, axis, [(i, (i + by) % count) for i in range(count)])


def neighbour_swapped(array):
    count = lax.axis_size("blk")
    return lax.ppermute(array, "blk", [(i, i ^ 1) for i in range(count)])


def direct_pairs():
    count = lax.axis_size("blk")
    return [(i, (i + (3 if i % 2 else 1)) % count) for i in range(count)]


def direct_step():
    return jnp.where(lax.axis_index("blk") % 2 == 0, 1, 3)


def table_rows(parts):
    return -(-3 * parts // 8) * 8


def doublings(reach):
    known, rounds = 0, []
    while known < reach:
        shift = min(2 * known + 1, reach - known)
        rounds.append((shift, known))
        known += shift
    return rounds


def known_places(reach):
    held = [[0]]
    for shift, known in doublings(reach):
        for centre in (shift, -shift):
            held.append(list(range(centre - known, centre + known + 1)))
    return held


def whole_axis_known(count):
    return power_of_two(count) and count <= 2 * STEPS


def slot_counts(parts):
    counts = [1]
    while sum(counts) < parts:
        counts.append(min(sum(counts), parts - sum(counts)))
    return counts


def inverse_norm(wide):
    return lax.rsqrt(jnp.sum(wide * wide, axis=-1, keepdims=True) + 1e-06)


def store_units(raws, out, base):
    for at in range(0, raws[0].shape[0], CHUNK):
        wide = sum(raw[at : at + CHUNK, :].astype(F32) for raw in raws)
        here = pl.multiple_of(base + at, CHUNK)
        out[pl.ds(here, CHUNK), :] = (wide * inverse_norm(wide)).astype(BF16)


def own_kernel(image, text, img_out, txt_out):
    store_units([image], img_out, 0)
    store_units([text], txt_out, 0)


def diagonal(rows):
    return lax.broadcasted_iota(jnp.int32, (rows, rows), 0) == lax.broadcasted_iota(
        jnp.int32, (rows, rows), 1
    )


def to_lanes(column, eye):
    return jnp.sum(jnp.where(eye, column, 0.0), axis=0, keepdims=True)


def to_column(lanes, eye):
    return jnp.sum(jnp.where(eye, lanes, 0.0), axis=1, keepdims=True)


def onehot_of(positive, eye, parts, rows):
    wanted = to_column(positive.astype(F32), eye)
    lane = lax.broadcasted_iota(jnp.int32, (rows, rows), 1)
    quarter = lax.axis_index("rep")
    return [wanted == (lane + place(quarter, s, parts) * rows).astype(F32) for s in range(parts)]


def scores_kernel(parts, slots, factor, positive, images, scores, txt_out, row_out, col_out):
    rows = positive.shape[1]
    eye = diagonal(rows)
    wanted = to_column(positive.astype(F32), eye)
    lane = lax.broadcasted_iota(jnp.int32, (rows, rows), 1)
    quarter = lax.axis_index("rep")
    scores[...] = factor * lax.dot_general(
        images[...], txt_out[...], (((1,), (1,)), ((), ())), preferred_element_type=F32
    )
    peaks, sums = [], []
    for k in range(STEPS):
        tile = scores[k * rows : (k + 1) * rows, :]
        peak = jnp.max(tile, axis=1, keepdims=True)
        peaks.append(to_lanes(peak, eye))
        sums.append(to_lanes(jnp.sum(jnp.exp(tile - peak), axis=1, keepdims=True), eye))
    found = jnp.zeros((rows, 1), F32)
    col_peaks, col_sums, picked = [], [], []
    for n, s in enumerate(slots):
        tile = scores[:, n * rows : (n + 1) * rows]
        peak = jnp.max(tile, axis=0, keepdims=True)
        col_peaks.append(peak)
        col_sums.append(jnp.sum(jnp.exp(tile - peak), axis=0, keepdims=True))
        match = wanted == (lane + place(quarter, s, parts) * rows).astype(F32)
        chosen = jnp.where(match, tile[:rows, :], 0.0)
        picked.append(jnp.sum(chosen, axis=0, keepdims=True))
        found = found + jnp.sum(chosen, axis=1, keepdims=True)
    row_out[...] = jnp.concatenate(peaks + sums + [to_lanes(found, eye)], axis=0)
    col_out[...] = jnp.concatenate(col_peaks + col_sums + picked, axis=0)


def first_kernel(parts, scale, positive, *refs):
    own_image, direct, second, other, own_text = refs[:5]
    texts = refs[5 : 5 + parts - 2]
    img_out, scores, txt_out, *stats = refs[5 + parts - 2 :]
    rows = own_image.shape[0]
    step = direct_step()
    img_out[:rows, :] = own_image[...]
    store_units([direct], img_out, step * rows)
    store_units([second], img_out, 2 * rows)
    store_units([other], img_out, (STEPS - step) * rows)
    txt_out[:rows, :] = own_text[...]
    for n, text in enumerate(texts):
        store_units([text], txt_out, (n + 1) * rows)
    slots = range(parts - 1)
    scores_kernel(parts, slots, scale[0], positive[...], img_out, scores, txt_out, *stats)


def last_kernel(parts, scale, positive, images, row_first, col_first, *refs):
    *texts, scores, txt_out, row_stats, col_stats, row_pos, row_last, col_last = refs
    store_units(texts, txt_out, 0)
    slots = [parts - 1]
    scores_kernel(
        parts, slots, scale[0], positive[...], images, scores, txt_out, row_last, col_last
    )
    peaks = jnp.maximum(row_first[:STEPS, :], row_last[:STEPS, :])
    sums = sum(
        t[STEPS : 2 * STEPS, :] * jnp.exp(t[:STEPS, :] - peaks) for t in (row_first, row_last)
    )
    row_stats[...] = jnp.concatenate([peaks, sums], axis=0)
    row_pos[...] = row_first[2 * STEPS :, :] + row_last[2 * STEPS :, :]
    tables = []
    for which in range(3):
        tables += [col_first[which * (parts - 1) : (which + 1) * (parts - 1), :]]
        tables += [col_last[which : which + 1, :]]
    blank = jnp.zeros((col_stats.shape[0] - 3 * parts, col_last.shape[1]), F32)
    col_stats[...] = jnp.concatenate(tables + [blank] * (blank.shape[0] > 0), axis=0)


def merged(pairs):
    peak = functools.reduce(jnp.maximum, [p for p, _ in pairs])
    return peak + jnp.log(sum(s * jnp.exp(p - peak) for p, s in pairs))


def row_table_lookup(refs, tables):
    height = 2 * STEPS
    at = 0
    for ref in refs:
        tables[at : at + ref.shape[0], :] = ref[...]
        at += ref.shape[0]
    if whole_axis_known(lax.axis_size("blk")):
        count = lax.axis_size("blk")
        own = lax.axis_index("blk")

        def lookup(shift):
            slot = own ^ ((own + shift + count) % count)
            return tables[pl.ds(pl.multiple_of(slot * height, height), height), :]

        return lookup
    order = [shift for held in known_places(STEPS - 1) for shift in held]
    return lambda shift: tables[pl.ds(order.index(shift) * height, height), :]


def weights_kernel(parts, n_rows, positive, first, last, images, row_pos, *refs):
    row_refs, refs = refs[:n_rows], refs[n_rows:]
    held = slot_counts(parts)
    col_refs, refs = refs[: len(held)], refs[len(held) :]
    row_loss, col_loss, weights, *txt_parts, row_scratch = refs
    rows = row_pos.shape[1]
    eye = diagonal(rows)
    onehot = onehot_of(positive[...], eye, parts, rows)
    row_table = row_table_lookup(row_refs, row_scratch)
    row_tables = {shift: row_table(shift) for shift in range(1 - STEPS, STEPS)}
    height = table_rows(parts)
    col_tables = []
    for ref, count in zip(col_refs, held):
        col_tables += [ref[n * height : (n + 1) * height, :] for n in range(count)]

    def row_pair(shift, k):
        table, at = row_tables[shift], k - shift
        return table[at : at + 1, :], table[STEPS + at : STEPS + at + 1, :]

    row_lse = []
    for k in range(STEPS):
        lse = merged([row_pair(t, k) for t in range(1 - STEPS, STEPS) if 0 <= k - t < STEPS])
        if k == 0:
            row_loss[...] = lse - row_pos[...]
        row_lse.append(to_column(lse, eye))
    col_lse = []
    for s in range(parts):
        at = [(col_tables[t], slot_at(s, t, parts)) for t in range(parts)]
        lse = merged([(c[q : q + 1, :], c[parts + q : parts + q + 1, :]) for c, q in at])
        if s == 0:
            col_loss[...] = lse - sum(c[2 * parts + q : 2 * parts + q + 1, :] for c, q in at)
        col_lse.append(lse)
    for s in range(parts):
        source, base = (first, s * rows) if s < parts - 1 else (last, 0)
        for k in range(STEPS):
            tile = source[k * rows : (k + 1) * rows, base : base + rows]
            weight = 0.5 * (jnp.exp(tile - row_lse[k]) + jnp.exp(tile - col_lse[s]))
            if k == 0:
                weight = weight - onehot[s].astype(F32)
            weights[k * rows : (k + 1) * rows, s * rows : (s + 1) * rows] = weight.astype(BF16)
    for s in range(parts):
        part = lax.dot_general(
            weights[:, s * rows : (s + 1) * rows],
            images[...],
            (((0,), (0,)), ((), ())),
            preferred_element_type=F32,
        )
        for out in txt_parts[2 * s : 2 * s + 2]:
            out[...] = part.astype(out.dtype)


def images_kernel(weights, first, last, own, direct, second, other):
    rows = own.shape[0]
    split = first.shape[0]
    step = direct_step()
    for out, k in ((other, STEPS - step), (direct, step), (second, 2), (own, 0)):
        strip = pl.ds(pl.multiple_of(k * rows, rows), rows)
        part = jnp.dot(weights[strip, :split], first[...], preferred_element_type=F32)
        part = part + jnp.dot(weights[strip, split:], last[...], preferred_element_type=F32)
        out[...] = part.astype(out.dtype)


def final_kernel(scale, raw, *refs):
    grad = refs[-1]
    factor = scale[0]
    for at in range(0, raw.shape[0], CHUNK):
        chunk = slice(at, at + CHUNK)
        wide = raw[chunk, :].astype(F32)
        inverse = inverse_norm(wide)
        unit = wide * inverse
        total = factor * sum(part[chunk, :].astype(F32) for part in refs[:-1])
        along = jnp.sum(unit * total, axis=-1, keepdims=True)
        grad[chunk, :] = (total - unit * along) * inverse


def call(kernel, outs, specs, args, scratch=()):
    return pl.pallas_call(
        kernel,
        out_shape=outs,
        in_specs=[pl.BlockSpec(memory_space=space) for space in specs],
        out_specs=jax.tree.map(lambda _: pl.BlockSpec(memory_space=VMEM), outs),
        scratch_shapes=list(scratch),
        compiler_params=pltpu.CompilerParams(vmem_limit_bytes=16 << 20),
    )(*args)


def is_line(parts):
    return parts == 4


def gathered_texts(text):
    parts = lax.axis_size("rep")
    if not is_line(parts):
        return [[fetched(text, "rep", s)] for s in range(1, parts)]
    from_ends = lax.ppermute(text, "rep", [(0, 2), (3, 1)])
    near = fetched(text, "rep", 1)
    to_ends = lax.ppermute(text, "rep", [(1, 3), (2, 0)])
    middle = lax.ppermute(text, "rep", [(1, 2), (2, 1)])
    onward = lax.ppermute(from_ends, "rep", [(2, 3), (1, 0)])
    return [[near], [from_ends, to_ends], [middle, onward]]


def returned_texts(parts_of):
    parts = len(parts_of)
    if not is_line(parts):
        return [returned(parts_of[s][1], "rep", s) for s in range(1, parts)]
    (_, near), (second, second_sent), (_, far) = parts_of[1:]
    early = lax.ppermute(far, "rep", [(0, 1), (3, 2)])
    middle = lax.ppermute(far, "rep", [(1, 2), (2, 1)])
    from_ends = lax.ppermute(second_sent, "rep", [(0, 2), (3, 1)])
    next_one = returned(near, "rep", 1)
    joined = (second + early.astype(F32)).astype(BF16)
    to_ends = lax.ppermute(joined, "rep", [(1, 3), (2, 0)])
    return [next_one, middle, from_ends, to_ends]


def gathered_images(image):
    direct = lax.ppermute(image, "blk", [(b, a) for a, b in direct_pairs()])
    second = passed_along(image, "blk", -2)
    return direct, second, neighbour_swapped(second)


def known_row_tables(own):
    count = lax.axis_size("blk")
    tables = [own]
    if whole_axis_known(count):
        while sum(t.shape[0] for t in tables) < count * own.shape[0]:
            sent = jnp.concatenate(tables, axis=0)
            n = len(tables) - 1
            tables.append(fetched(sent, "blk", 2**n))
        return tables
    for n, (shift, known) in enumerate(doublings(STEPS - 1)):
        by_shift = {}
        for array, shifts in zip(tables, known_places(STEPS - 1)):
            for at, shifted in enumerate(shifts):
                by_shift[shifted] = array[at * 2 * STEPS : (at + 1) * 2 * STEPS]
        sent = jnp.concatenate([by_shift[t] for t in range(-known, known + 1)], axis=0)
        for sign in (1, -1):
            tables.append(passed_along(sent, "blk", -sign * shift))
    return tables


def on_device(image, text, positive, logit_scale):
    rows, width = image.shape
    parts = lax.axis_size("rep")
    height = table_rows(parts)
    shape = jax.ShapeDtypeStruct
    *texts, text_last = gathered_texts(text)
    direct, second, other = gathered_images(image)
    own_image, own_text = call(
        own_kernel, [shape((rows, width), BF16)] * 2, [VMEM] * 2, (image, text)
    )
    split = (parts - 1) * rows
    joined_texts = [sum(arrays[1:], arrays[0]) for arrays in texts]
    img_tiles, first, txt_first, row_first, col_first = call(
        functools.partial(first_kernel, parts),
        (
            shape((STEPS * rows, width), BF16),
            shape((STEPS * rows, split), F32),
            shape((split, width), BF16),
            shape((2 * STEPS + 1, rows), F32),
            shape((3 * (parts - 1), rows), F32),
        ),
        [SMEM] + [VMEM] * (6 + len(joined_texts)),
        (logit_scale, positive, own_image, direct, second, other, own_text, *joined_texts),
    )
    last, txt_last, row_stats, col_stats, row_pos = call(
        functools.partial(last_kernel, parts),
        (
            shape((STEPS * rows, rows), F32),
            shape((rows, width), BF16),
            shape((2 * STEPS, rows), F32),
            shape((height, rows), F32),
            shape((1, rows), F32),
        ),
        [SMEM] + [VMEM] * (4 + len(text_last)),
        (logit_scale, positive, img_tiles, row_first, col_first, *text_last),
        [pltpu.VMEM((2 * STEPS + 1, rows), F32), pltpu.VMEM((3, rows), F32)],
    )
    col_tables = [col_stats]
    for n, count in enumerate(slot_counts(parts)[1:]):
        sent = jnp.concatenate(col_tables, axis=0)[: count * height]
        col_tables.append(fetched(sent, "rep", 2**n))
    row_tables = known_row_tables(row_stats)
    row_loss, col_loss, weights, *txt_parts = call(
        functools.partial(weights_kernel, parts, len(row_tables)),
        (
            shape((1, rows), F32),
            shape((1, rows), F32),
            shape((STEPS * rows, parts * rows), BF16),
            *[shape((rows, width), t) for _ in range(parts) for t in (F32, BF16)],
        ),
        [VMEM] * (5 + len(row_tables) + len(col_tables)),
        (positive, first, last, img_tiles, row_pos, *row_tables, *col_tables),
        [pltpu.VMEM((sum(t.shape[0] for t in row_tables), rows), F32)],
    )
    txt_parts = list(zip(txt_parts[::2], txt_parts[1::2]))
    txt_sums = [txt_parts[0][0], *returned_texts(txt_parts)]
    own, direct, second, other = call(
        images_kernel,
        [shape((rows, width), t) for t in (F32, BF16, F32, BF16)],
        [VMEM] * 3,
        (weights, txt_first, txt_last),
    )
    swapped = neighbour_swapped(other)
    joined = (second + swapped.astype(F32)).astype(BF16)
    img_sums = [own, lax.ppermute(direct, "blk", direct_pairs()), passed_along(joined, "blk", 2)]
    grads = [
        call(
            final_kernel,
            shape((rows, width), F32),
            [SMEM] + [VMEM] * (1 + len(sums)),
            (logit_scale, raw, *sums),
        )
        for raw, sums in ((image, img_sums), (text, txt_sums))
    ]
    return (row_loss[0], col_loss[0], *grads)


def solution(mesh):
    placed = (P(("blk", "rep"), None), P(("blk", "rep"), None), P("blk", "rep"), P())

    return jax.shard_map(
        on_device,
        mesh=mesh,
        in_specs=placed,
        out_specs=(
            P(("blk", "rep")),
            P(("blk", "rep")),
            P(("blk", "rep"), None),
            P(("blk", "rep"), None),
        ),
        check_vma=False,
    )
```

```python
import functools

import jax
import jax.numpy as jnp
from jax import lax
from jax.experimental import pallas as pl
from jax.experimental.pallas import tpu as pltpu
from jax.sharding import PartitionSpec as P

STEPS = 4
CHUNK = 16
F32 = jnp.float32
BF16 = jnp.bfloat16
VMEM = pltpu.VMEM
SMEM = pltpu.SMEM


def power_of_two(count):
    return count & (count - 1) == 0


def place(own, slot, count):
    return own ^ slot if power_of_two(count) else (own + slot) % count


def slot_at(slot, partner, count):
    return slot ^ partner if power_of_two(count) else (slot - partner) % count


def fetched(array, axis, slot):
    count = lax.axis_size(axis)
    return lax.ppermute(array, axis, [(place(i, slot, count), i) for i in range(count)])


def returned(array, axis, slot):
    count = lax.axis_size(axis)
    return lax.ppermute(array, axis, [(i, place(i, slot, count)) for i in range(count)])


def passed_along(array, axis, by):
    count = lax.axis_size(axis)
    return lax.ppermute(array, axis, [(i, (i + by) % count) for i in range(count)])


def neighbour_swapped(array):
    count = lax.axis_size("blk")
    return lax.ppermute(array, "blk", [(i, i ^ 1) for i in range(count)])


def direct_pairs():
    count = lax.axis_size("blk")
    return [(i, (i + (3 if i % 2 else 1)) % count) for i in range(count)]


def direct_step():
    return jnp.where(lax.axis_index("blk") % 2 == 0, 1, 3)


def table_rows(parts):
    return -(-3 * parts // 8) * 8


def doublings(reach):
    known, rounds = 0, []
    while known < reach:
        shift = min(2 * known + 1, reach - known)
        rounds.append((shift, known))
        known += shift
    return rounds


def known_places(reach):
    held = [[0]]
    for shift, known in doublings(reach):
        for centre in (shift, -shift):
            held.append(list(range(centre - known, centre + known + 1)))
    return held


def whole_axis_known(count):
    return power_of_two(count) and count <= 2 * STEPS


def slot_counts(parts):
    counts = [1]
    while sum(counts) < parts:
        counts.append(min(sum(counts), parts - sum(counts)))
    return counts


def inverse_norm(wide):
    return lax.rsqrt(jnp.sum(wide * wide, axis=-1, keepdims=True) + 1e-06)


def store_units(raw, out, base):
    for at in range(0, raw.shape[0], CHUNK):
        wide = raw[at : at + CHUNK, :].astype(F32)
        here = pl.multiple_of(base + at, CHUNK)
        out[pl.ds(here, CHUNK), :] = (wide * inverse_norm(wide)).astype(BF16)


def own_kernel(image, text, img_out, txt_out):
    store_units(image, img_out, 0)
    store_units(text, txt_out, 0)


def diagonal(rows):
    return lax.broadcasted_iota(jnp.int32, (rows, rows), 0) == lax.broadcasted_iota(
        jnp.int32, (rows, rows), 1
    )


def to_lanes(column, eye):
    return jnp.sum(jnp.where(eye, column, 0.0), axis=0, keepdims=True)


def to_column(lanes, eye):
    return jnp.sum(jnp.where(eye, lanes, 0.0), axis=1, keepdims=True)


def onehot_of(positive, eye, parts, rows):
    wanted = to_column(positive.astype(F32), eye)
    lane = lax.broadcasted_iota(jnp.int32, (rows, rows), 1)
    quarter = lax.axis_index("rep")
    return [wanted == (lane + place(quarter, s, parts) * rows).astype(F32) for s in range(parts)]


def scores_kernel(parts, slots, factor, positive, images, scores, txt_out, row_out, col_out):
    rows = positive.shape[1]
    eye = diagonal(rows)
    wanted = to_column(positive.astype(F32), eye)
    lane = lax.broadcasted_iota(jnp.int32, (rows, rows), 1)
    quarter = lax.axis_index("rep")
    scores[...] = factor * lax.dot_general(
        images[...], txt_out[...], (((1,), (1,)), ((), ())), preferred_element_type=F32
    )
    peaks, sums = [], []
    for k in range(STEPS):
        tile = scores[k * rows : (k + 1) * rows, :]
        peak = jnp.max(tile, axis=1, keepdims=True)
        peaks.append(to_lanes(peak, eye))
        sums.append(to_lanes(jnp.sum(jnp.exp(tile - peak), axis=1, keepdims=True), eye))
    found = jnp.zeros((rows, 1), F32)
    col_peaks, col_sums, picked = [], [], []
    for n, s in enumerate(slots):
        tile = scores[:, n * rows : (n + 1) * rows]
        peak = jnp.max(tile, axis=0, keepdims=True)
        col_peaks.append(peak)
        col_sums.append(jnp.sum(jnp.exp(tile - peak), axis=0, keepdims=True))
        match = wanted == (lane + place(quarter, s, parts) * rows).astype(F32)
        chosen = jnp.where(match, tile[:rows, :], 0.0)
        picked.append(jnp.sum(chosen, axis=0, keepdims=True))
        found = found + jnp.sum(chosen, axis=1, keepdims=True)
    row_out[...] = jnp.concatenate(peaks + sums + [to_lanes(found, eye)], axis=0)
    col_out[...] = jnp.concatenate(col_peaks + col_sums + picked, axis=0)


def first_kernel(parts, scale, positive, *refs):
    own_image, direct, second, other, own_text = refs[:5]
    texts = refs[5 : 5 + parts - 2]
    img_out, scores, txt_out, *stats = refs[5 + parts - 2 :]
    rows = own_image.shape[0]
    step = direct_step()
    img_out[:rows, :] = own_image[...]
    store_units(direct, img_out, step * rows)
    store_units(second, img_out, 2 * rows)
    store_units(other, img_out, (STEPS - step) * rows)
    txt_out[:rows, :] = own_text[...]
    for slot, text in zip(near_slots(parts), texts):
        store_units(text, txt_out, slot * rows)
    slots = range(parts - 1)
    scores_kernel(parts, slots, scale[0], positive[...], img_out, scores, txt_out, *stats)


def last_kernel(parts, scale, positive, images, row_first, col_first, *refs):
    *texts, scores, txt_out, row_stats, col_stats, row_pos, row_last, col_last = refs
    if len(texts) == 1:
        store_units(texts[0], txt_out, 0)
    else:
        end = at_end(parts)
        pl.when(end)(lambda: store_units(texts[0], txt_out, 0))
        pl.when(jnp.logical_not(end))(lambda: store_units(texts[1], txt_out, 0))
    slots = [parts - 1]
    scores_kernel(
        parts, slots, scale[0], positive[...], images, scores, txt_out, row_last, col_last
    )
    peaks = jnp.maximum(row_first[:STEPS, :], row_last[:STEPS, :])
    sums = sum(
        t[STEPS : 2 * STEPS, :] * jnp.exp(t[:STEPS, :] - peaks) for t in (row_first, row_last)
    )
    row_stats[...] = jnp.concatenate([peaks, sums], axis=0)
    row_pos[...] = row_first[2 * STEPS :, :] + row_last[2 * STEPS :, :]
    tables = []
    for which in range(3):
        tables += [col_first[which * (parts - 1) : (which + 1) * (parts - 1), :]]
        tables += [col_last[which : which + 1, :]]
    blank = jnp.zeros((col_stats.shape[0] - 3 * parts, col_last.shape[1]), F32)
    col_stats[...] = jnp.concatenate(tables + [blank] * (blank.shape[0] > 0), axis=0)


def merged(pairs):
    peak = functools.reduce(jnp.maximum, [p for p, _ in pairs])
    return peak + jnp.log(sum(s * jnp.exp(p - peak) for p, s in pairs))


def row_table_lookup(refs, tables):
    height = 2 * STEPS
    at = 0
    for ref in refs:
        tables[at : at + ref.shape[0], :] = ref[...]
        at += ref.shape[0]
    if whole_axis_known(lax.axis_size("blk")):
        count = lax.axis_size("blk")
        own = lax.axis_index("blk")

        def lookup(shift):
            slot = own ^ ((own + shift + count) % count)
            return tables[pl.ds(pl.multiple_of(slot * height, height), height), :]

        return lookup
    order = [shift for held in known_places(STEPS - 1) for shift in held]
    return lambda shift: tables[pl.ds(order.index(shift) * height, height), :]


def weights_kernel(parts, n_rows, positive, first, last, images, txt_first, txt_last, row_pos, *refs):
    row_refs, refs = refs[:n_rows], refs[n_rows:]
    held = slot_counts(parts)
    col_refs, refs = refs[: len(held)], refs[len(held) :]
    row_loss, col_loss, weights, other, *narrow, row_scratch = refs
    rows = row_pos.shape[1]
    eye = diagonal(rows)
    onehot = onehot_of(positive[...], eye, parts, rows)
    row_table = row_table_lookup(row_refs, row_scratch)
    row_tables = {shift: row_table(shift) for shift in range(1 - STEPS, STEPS)}
    height = table_rows(parts)
    col_tables = []
    for ref, count in zip(col_refs, held):
        col_tables += [ref[n * height : (n + 1) * height, :] for n in range(count)]

    def row_pair(shift, k):
        table, at = row_tables[shift], k - shift
        return table[at : at + 1, :], table[STEPS + at : STEPS + at + 1, :]

    row_lse = []
    for k in range(STEPS):
        lse = merged([row_pair(t, k) for t in range(1 - STEPS, STEPS) if 0 <= k - t < STEPS])
        if k == 0:
            row_loss[...] = lse - row_pos[...]
        row_lse.append(to_column(lse, eye))
    col_lse = []
    for s in range(parts):
        at = [(col_tables[t], slot_at(s, t, parts)) for t in range(parts)]
        lse = merged([(c[q : q + 1, :], c[parts + q : parts + q + 1, :]) for c, q in at])
        if s == 0:
            col_loss[...] = lse - sum(c[2 * parts + q : 2 * parts + q + 1, :] for c, q in at)
        col_lse.append(lse)
    for s in range(parts):
        source, base = (first, s * rows) if s < parts - 1 else (last, 0)
        for k in range(STEPS):
            tile = source[k * rows : (k + 1) * rows, base : base + rows]
            weight = 0.5 * (jnp.exp(tile - row_lse[k]) + jnp.exp(tile - col_lse[s]))
            if k == 0:
                weight = weight - onehot[s].astype(F32)
            weights[k * rows : (k + 1) * rows, s * rows : (s + 1) * rows] = weight.astype(BF16)
    for slot, out in zip(sent_slots(parts)[0], narrow):
        text_part(weights, images, slot, out)
    other[...] = image_part(weights, txt_first, txt_last, STEPS - direct_step(), rows).astype(BF16)


def text_part(weights, images, slot, out):
    rows = out.shape[0]
    strip = pl.ds(pl.multiple_of(slot * rows, rows), rows)
    part = lax.dot_general(
        weights[:, strip], images[...], (((0,), (0,)), ((), ())), preferred_element_type=F32
    )
    out[...] = part.astype(out.dtype)


def image_part(weights, first, last, k, rows):
    strip = pl.ds(pl.multiple_of(k * rows, rows), rows)
    split = first.shape[0]
    part = jnp.dot(weights[strip, :split], first[...], preferred_element_type=F32)
    return part + jnp.dot(weights[strip, split:], last[...], preferred_element_type=F32)


def rest_kernel(parts, weights, images, first, last, swapped, own, direct, second, *kept):
    rows = own.shape[0]
    joined = image_part(weights, first, last, 2, rows) + swapped[...].astype(F32)
    second[...] = joined.astype(BF16)
    direct[...] = image_part(weights, first, last, direct_step(), rows).astype(BF16)
    own[...] = image_part(weights, first, last, 0, rows)
    for slot, out in zip(sent_slots(parts)[1], kept):
        text_part(weights, images, slot, out)


def join_kernel(parts, kept, arrived, joined):
    end = at_end(parts)
    for at in range(0, kept.shape[0], CHUNK):
        chunk = slice(at, at + CHUNK)
        added = jnp.where(end, 0.0, arrived[chunk, :].astype(F32))
        joined[chunk, :] = (kept[chunk, :] + added).astype(BF16)


def final_kernel(n_always, n_end, parts, scale, raw, *refs):
    *refs, grad = refs
    always, ends, others = refs[:n_always], refs[n_always : n_always + n_end], refs[n_always + n_end :]
    factor = scale[0]
    end = at_end(parts)
    for at in range(0, raw.shape[0], CHUNK):
        chunk = slice(at, at + CHUNK)
        wide = raw[chunk, :].astype(F32)
        inverse = inverse_norm(wide)
        unit = wide * inverse
        total = sum(part[chunk, :].astype(F32) for part in always)
        if ends:
            at_ends = sum(part[chunk, :].astype(F32) for part in ends)
            total += jnp.where(end, at_ends, sum(part[chunk, :].astype(F32) for part in others))
        total = factor * total
        along = jnp.sum(unit * total, axis=-1, keepdims=True)
        grad[chunk, :] = (total - unit * along) * inverse


def call(kernel, outs, specs, args, scratch=()):
    return pl.pallas_call(
        kernel,
        out_shape=outs,
        in_specs=[pl.BlockSpec(memory_space=space) for space in specs],
        out_specs=jax.tree.map(lambda _: pl.BlockSpec(memory_space=VMEM), outs),
        scratch_shapes=list(scratch),
        compiler_params=pltpu.CompilerParams(vmem_limit_bytes=16 << 20),
    )(*args)


def is_line(parts):
    return parts == 4


def at_end(parts):
    quarter = lax.axis_index("rep")
    return (quarter == 0) | (quarter == parts - 1)


def near_slots(parts):
    if not is_line(parts):
        return list(range(1, parts - 1))
    first = jnp.where(at_end(parts), 1, 2)
    return [first, 3 - first]


def sent_slots(parts):
    if not is_line(parts):
        return list(range(1, parts)), [0]
    end = at_end(parts)
    return [jnp.where(end, 3, 1), jnp.where(end, 2, 3)], [0, jnp.where(end, 1, 2)]


def gathered_texts(text):
    parts = lax.axis_size("rep")
    if not is_line(parts):
        texts = [fetched(text, "rep", s) for s in range(1, parts)]
        return texts[:-1], texts[-1:]
    one = lax.ppermute(text, "rep", [(0, 2), (3, 1), (1, 0), (2, 3)])
    two = lax.ppermute(text, "rep", [(0, 1), (3, 2), (1, 3), (2, 0)])
    middle = lax.ppermute(text, "rep", [(1, 2), (2, 1), (0, 0), (3, 3)])
    onward = lax.ppermute(one, "rep", [(1, 0), (2, 3), (0, 1), (3, 2)])
    return [one, two], [onward, middle]


def returned_texts(narrow, kept):
    parts = lax.axis_size("rep")
    if not is_line(parts):
        back = [returned(part, "rep", s) for s, part in enumerate(narrow, 1)]
        return [kept[0], *back], [], []
    early, late = narrow
    one = lax.ppermute(early, "rep", [(0, 1), (3, 2), (1, 0), (2, 3)])
    middle = lax.ppermute(late, "rep", [(1, 2), (2, 1), (0, 0), (3, 3)])
    ends = lax.ppermute(late, "rep", [(0, 2), (3, 1), (1, 0), (2, 3)])
    joined = call(
        functools.partial(join_kernel, parts),
        jax.ShapeDtypeStruct(one.shape, BF16),
        [VMEM] * 2,
        (kept[1], one),
    )
    joined = lax.ppermute(joined, "rep", [(0, 1), (3, 2), (1, 3), (2, 0)])
    return [kept[0], joined], [one], [middle, ends]


def gathered_images(image):
    direct = lax.ppermute(image, "blk", [(b, a) for a, b in direct_pairs()])
    second = passed_along(image, "blk", -2)
    return direct, second, neighbour_swapped(second)


def known_row_tables(own):
    count = lax.axis_size("blk")
    tables = [own]
    if whole_axis_known(count):
        while sum(t.shape[0] for t in tables) < count * own.shape[0]:
            sent = jnp.concatenate(tables, axis=0)
            n = len(tables) - 1
            tables.append(fetched(sent, "blk", 2**n))
        return tables
    for n, (shift, known) in enumerate(doublings(STEPS - 1)):
        by_shift = {}
        for array, shifts in zip(tables, known_places(STEPS - 1)):
            for at, shifted in enumerate(shifts):
                by_shift[shifted] = array[at * 2 * STEPS : (at + 1) * 2 * STEPS]
        sent = jnp.concatenate([by_shift[t] for t in range(-known, known + 1)], axis=0)
        for sign in (1, -1):
            tables.append(passed_along(sent, "blk", -sign * shift))
    return tables


def on_device(image, text, positive, logit_scale):
    rows, width = image.shape
    parts = lax.axis_size("rep")
    height = table_rows(parts)
    shape = jax.ShapeDtypeStruct
    texts, text_last = gathered_texts(text)
    direct, second, other = gathered_images(image)
    own_image, own_text = call(
        own_kernel, [shape((rows, width), BF16)] * 2, [VMEM] * 2, (image, text)
    )
    split = (parts - 1) * rows
    img_tiles, first, txt_first, row_first, col_first = call(
        functools.partial(first_kernel, parts),
        (
            shape((STEPS * rows, width), BF16),
            shape((STEPS * rows, split), F32),
            shape((split, width), BF16),
            shape((2 * STEPS + 1, rows), F32),
            shape((3 * (parts - 1), rows), F32),
        ),
        [SMEM] + [VMEM] * (6 + len(texts)),
        (logit_scale, positive, own_image, direct, second, other, own_text, *texts),
    )
    last, txt_last, row_stats, col_stats, row_pos = call(
        functools.partial(last_kernel, parts),
        (
            shape((STEPS * rows, rows), F32),
            shape((rows, width), BF16),
            shape((2 * STEPS, rows), F32),
            shape((height, rows), F32),
            shape((1, rows), F32),
        ),
        [SMEM] + [VMEM] * (4 + len(text_last)),
        (logit_scale, positive, img_tiles, row_first, col_first, *text_last),
        [pltpu.VMEM((2 * STEPS + 1, rows), F32), pltpu.VMEM((3, rows), F32)],
    )
    col_tables = [col_stats]
    for n, count in enumerate(slot_counts(parts)[1:]):
        sent = jnp.concatenate(col_tables, axis=0)[: count * height]
        col_tables.append(fetched(sent, "rep", 2**n))
    row_tables = known_row_tables(row_stats)
    narrow_slots, kept_slots = sent_slots(parts)
    row_loss, col_loss, weights, other, *narrow = call(
        functools.partial(weights_kernel, parts, len(row_tables)),
        (
            shape((1, rows), F32),
            shape((1, rows), F32),
            shape((STEPS * rows, parts * rows), BF16),
            *[shape((rows, width), BF16) for _ in range(1 + len(narrow_slots))],
        ),
        [VMEM] * (7 + len(row_tables) + len(col_tables)),
        (
            positive,
            first,
            last,
            img_tiles,
            txt_first,
            txt_last,
            row_pos,
            *row_tables,
            *col_tables,
        ),
        [pltpu.VMEM((sum(t.shape[0] for t in row_tables), rows), F32)],
    )
    swapped = neighbour_swapped(other)
    own, direct, second, *kept = call(
        functools.partial(rest_kernel, parts),
        [shape((rows, width), t) for t in (F32, BF16, BF16, *[F32 for _ in kept_slots])],
        [VMEM] * 5,
        (weights, img_tiles, txt_first, txt_last, swapped),
    )
    img_sums = [own, lax.ppermute(direct, "blk", direct_pairs()), passed_along(second, "blk", 2)]
    txt_sums = returned_texts(narrow, kept)
    grads = []
    for raw, (always, ends, others) in ((image, (img_sums, [], [])), (text, txt_sums)):
        sums = [*always, *ends, *others]
        grads.append(
            call(
                functools.partial(final_kernel, len(always), len(ends), parts),
                shape((rows, width), F32),
                [SMEM] + [VMEM] * (1 + len(sums)),
                (logit_scale, raw, *sums),
            )
        )
    return (row_loss[0], col_loss[0], *grads)


def solution(mesh):
    placed = (P(("blk", "rep"), None), P(("blk", "rep"), None), P("blk", "rep"), P())

    return jax.shard_map(
        on_device,
        mesh=mesh,
        in_specs=placed,
        out_specs=(
            P(("blk", "rep")),
            P(("blk", "rep")),
            P(("blk", "rep"), None),
            P(("blk", "rep"), None),
        ),
        check_vma=False,
    )
```

```python
import functools

import jax
import jax.numpy as jnp
from jax import lax
from jax.experimental import pallas as pl
from jax.experimental.pallas import tpu as pltpu
from jax.sharding import PartitionSpec as P

STEPS = 4
CHUNK = 16
F32 = jnp.float32
BF16 = jnp.bfloat16
VMEM = pltpu.VMEM
SMEM = pltpu.SMEM


def power_of_two(count):
    return count & (count - 1) == 0


def place(own, slot, count):
    return own ^ slot if power_of_two(count) else (own + slot) % count


def slot_at(slot, partner, count):
    return slot ^ partner if power_of_two(count) else (slot - partner) % count


def fetched(array, axis, slot):
    count = lax.axis_size(axis)
    return lax.ppermute(array, axis, [(place(i, slot, count), i) for i in range(count)])


def returned(array, axis, slot):
    count = lax.axis_size(axis)
    return lax.ppermute(array, axis, [(i, place(i, slot, count)) for i in range(count)])


def passed_along(array, axis, by):
    count = lax.axis_size(axis)
    return lax.ppermute(array, axis, [(i, (i + by) % count) for i in range(count)])


def middle_swapped(array):
    parts, blocks = lax.axis_size("rep"), lax.axis_size("blk")
    pairs = [
        (b * parts + r, b * parts + parts - 1 - r if 0 < r < parts - 1 else (b ^ 1) * parts + r)
        for b in range(blocks)
        for r in range(parts)
    ]
    return lax.ppermute(array, ("blk", "rep"), pairs)


def neighbour_swapped(array):
    count = lax.axis_size("blk")
    return lax.ppermute(array, "blk", [(i, i ^ 1) for i in range(count)])


def direct_pairs():
    count = lax.axis_size("blk")
    return [(i, (i + (3 if i % 2 else 1)) % count) for i in range(count)]


def direct_step():
    return jnp.where(lax.axis_index("blk") % 2 == 0, 1, 3)


def table_rows(parts):
    return -(-3 * parts // 8) * 8


def doublings(reach):
    known, rounds = 0, []
    while known < reach:
        shift = min(2 * known + 1, reach - known)
        rounds.append((shift, known))
        known += shift
    return rounds


def known_places(reach):
    held = [[0]]
    for shift, known in doublings(reach):
        for centre in (shift, -shift):
            held.append(list(range(centre - known, centre + known + 1)))
    return held


def whole_axis_known(count):
    return power_of_two(count) and count <= 2 * STEPS


def slot_counts(parts):
    counts = [1]
    while sum(counts) < parts:
        counts.append(min(sum(counts), parts - sum(counts)))
    return counts


def inverse_norm(wide):
    return lax.rsqrt(jnp.sum(wide * wide, axis=-1, keepdims=True) + 1e-06)


def store_units(raw, out, base):
    for at in range(0, raw.shape[0], CHUNK):
        wide = raw[at : at + CHUNK, :].astype(F32)
        here = pl.multiple_of(base + at, CHUNK)
        out[pl.ds(here, CHUNK), :] = (wide * inverse_norm(wide)).astype(BF16)


def own_kernel(image, text, img_out, txt_out):
    store_units(image, img_out, 0)
    store_units(text, txt_out, 0)


def diagonal(rows):
    return lax.broadcasted_iota(jnp.int32, (rows, rows), 0) == lax.broadcasted_iota(
        jnp.int32, (rows, rows), 1
    )


def to_lanes(column, eye):
    return jnp.sum(jnp.where(eye, column, 0.0), axis=0, keepdims=True)


def to_column(lanes, eye):
    return jnp.sum(jnp.where(eye, lanes, 0.0), axis=1, keepdims=True)


def onehot_of(positive, eye, parts, rows):
    wanted = to_column(positive.astype(F32), eye)
    lane = lax.broadcasted_iota(jnp.int32, (rows, rows), 1)
    quarter = lax.axis_index("rep")
    return [wanted == (lane + place(quarter, s, parts) * rows).astype(F32) for s in range(parts)]


def scores_kernel(parts, slots, factor, positive, images, scores, txt_out, row_out, col_out):
    rows = positive.shape[1]
    eye = diagonal(rows)
    wanted = to_column(positive.astype(F32), eye)
    lane = lax.broadcasted_iota(jnp.int32, (rows, rows), 1)
    quarter = lax.axis_index("rep")
    scores[...] = factor * lax.dot_general(
        images[...], txt_out[...], (((1,), (1,)), ((), ())), preferred_element_type=F32
    )
    peaks, sums = [], []
    for k in range(STEPS):
        tile = scores[k * rows : (k + 1) * rows, :]
        peak = jnp.max(tile, axis=1, keepdims=True)
        peaks.append(to_lanes(peak, eye))
        sums.append(to_lanes(jnp.sum(jnp.exp(tile - peak), axis=1, keepdims=True), eye))
    found = jnp.zeros((rows, 1), F32)
    col_peaks, col_sums, picked = [], [], []
    for n, s in enumerate(slots):
        tile = scores[:, n * rows : (n + 1) * rows]
        peak = jnp.max(tile, axis=0, keepdims=True)
        col_peaks.append(peak)
        col_sums.append(jnp.sum(jnp.exp(tile - peak), axis=0, keepdims=True))
        match = wanted == (lane + place(quarter, s, parts) * rows).astype(F32)
        chosen = jnp.where(match, tile[:rows, :], 0.0)
        picked.append(jnp.sum(chosen, axis=0, keepdims=True))
        found = found + jnp.sum(chosen, axis=1, keepdims=True)
    row_out[...] = jnp.concatenate(peaks + sums + [to_lanes(found, eye)], axis=0)
    col_out[...] = jnp.concatenate(col_peaks + col_sums + picked, axis=0)


def first_kernel(parts, scale, positive, *refs):
    own_image, direct, second, other, own_text = refs[:5]
    texts = refs[5 : 5 + parts - 2]
    img_out, scores, txt_out, *stats = refs[5 + parts - 2 :]
    rows = own_image.shape[0]
    step = direct_step()
    img_out[:rows, :] = own_image[...]
    store_units(direct, img_out, step * rows)
    store_units(second, img_out, 2 * rows)
    store_units(other, img_out, (STEPS - step) * rows)
    txt_out[:rows, :] = own_text[...]
    for slot, text in zip(near_slots(parts), texts):
        store_units(text, txt_out, slot * rows)
    slots = range(parts - 1)
    scores_kernel(parts, slots, scale[0], positive[...], img_out, scores, txt_out, *stats)


def last_kernel(parts, scale, positive, images, row_first, col_first, *refs):
    *texts, scores, txt_out, row_stats, col_stats, row_pos, row_last, col_last = refs
    if len(texts) == 1:
        store_units(texts[0], txt_out, 0)
    else:
        end = at_end(parts)
        pl.when(end)(lambda: store_units(texts[0], txt_out, 0))
        pl.when(jnp.logical_not(end))(lambda: store_units(texts[1], txt_out, 0))
    slots = [parts - 1]
    scores_kernel(
        parts, slots, scale[0], positive[...], images, scores, txt_out, row_last, col_last
    )
    peaks = jnp.maximum(row_first[:STEPS, :], row_last[:STEPS, :])
    sums = sum(
        t[STEPS : 2 * STEPS, :] * jnp.exp(t[:STEPS, :] - peaks) for t in (row_first, row_last)
    )
    row_stats[...] = jnp.concatenate([peaks, sums], axis=0)
    row_pos[...] = row_first[2 * STEPS :, :] + row_last[2 * STEPS :, :]
    tables = []
    for which in range(3):
        tables += [col_first[which * (parts - 1) : (which + 1) * (parts - 1), :]]
        tables += [col_last[which : which + 1, :]]
    blank = jnp.zeros((col_stats.shape[0] - 3 * parts, col_last.shape[1]), F32)
    col_stats[...] = jnp.concatenate(tables + [blank] * (blank.shape[0] > 0), axis=0)


def merged(pairs):
    peak = functools.reduce(jnp.maximum, [p for p, _ in pairs])
    return peak + jnp.log(sum(s * jnp.exp(p - peak) for p, s in pairs))


def row_table_lookup(refs, tables):
    height = 2 * STEPS
    at = 0
    for ref in refs:
        tables[at : at + ref.shape[0], :] = ref[...]
        at += ref.shape[0]
    if whole_axis_known(lax.axis_size("blk")):
        count = lax.axis_size("blk")
        own = lax.axis_index("blk")

        def lookup(shift):
            slot = own ^ ((own + shift + count) % count)
            return tables[pl.ds(pl.multiple_of(slot * height, height), height), :]

        return lookup
    order = [shift for held in known_places(STEPS - 1) for shift in held]
    return lambda shift: tables[pl.ds(order.index(shift) * height, height), :]


def weights_kernel(parts, n_rows, positive, first, last, images, txt_first, txt_last, row_pos, *refs):
    row_refs, refs = refs[:n_rows], refs[n_rows:]
    held = slot_counts(parts)
    col_refs, refs = refs[: len(held)], refs[len(held) :]
    row_loss, col_loss, weights, other, *narrow, row_scratch = refs
    rows = row_pos.shape[1]
    eye = diagonal(rows)
    onehot = onehot_of(positive[...], eye, parts, rows)
    row_table = row_table_lookup(row_refs, row_scratch)
    row_tables = {shift: row_table(shift) for shift in range(1 - STEPS, STEPS)}
    height = table_rows(parts)
    col_tables = []
    for ref, count in zip(col_refs, held):
        col_tables += [ref[n * height : (n + 1) * height, :] for n in range(count)]

    def row_pair(shift, k):
        table, at = row_tables[shift], k - shift
        return table[at : at + 1, :], table[STEPS + at : STEPS + at + 1, :]

    row_lse = []
    for k in range(STEPS):
        lse = merged([row_pair(t, k) for t in range(1 - STEPS, STEPS) if 0 <= k - t < STEPS])
        if k == 0:
            row_loss[...] = lse - row_pos[...]
        row_lse.append(to_column(lse, eye))
    col_lse = []
    for s in range(parts):
        at = [(col_tables[t], slot_at(s, t, parts)) for t in range(parts)]
        lse = merged([(c[q : q + 1, :], c[parts + q : parts + q + 1, :]) for c, q in at])
        if s == 0:
            col_loss[...] = lse - sum(c[2 * parts + q : 2 * parts + q + 1, :] for c, q in at)
        col_lse.append(lse)
    for s in range(parts):
        source, base = (first, s * rows) if s < parts - 1 else (last, 0)
        for k in range(STEPS):
            tile = source[k * rows : (k + 1) * rows, base : base + rows]
            weight = 0.5 * (jnp.exp(tile - row_lse[k]) + jnp.exp(tile - col_lse[s]))
            if k == 0:
                weight = weight - onehot[s].astype(F32)
            weights[k * rows : (k + 1) * rows, s * rows : (s + 1) * rows] = weight.astype(BF16)
    for slot, out in zip(sent_slots(parts)[0], narrow):
        text_part(weights, images, slot, out)
    other[...] = image_part(weights, txt_first, txt_last, STEPS - direct_step(), rows).astype(BF16)


def text_part(weights, images, slot, out):
    rows = out.shape[0]
    strip = pl.ds(pl.multiple_of(slot * rows, rows), rows)
    part = lax.dot_general(
        weights[:, strip], images[...], (((0,), (0,)), ((), ())), preferred_element_type=F32
    )
    out[...] = part.astype(out.dtype)


def image_part(weights, first, last, k, rows):
    strip = pl.ds(pl.multiple_of(k * rows, rows), rows)
    split = first.shape[0]
    part = jnp.dot(weights[strip, :split], first[...], preferred_element_type=F32)
    return part + jnp.dot(weights[strip, split:], last[...], preferred_element_type=F32)


def rest_kernel(parts, weights, images, first, last, swapped, own, direct, second, *kept):
    rows = own.shape[0]
    joined = image_part(weights, first, last, 2, rows) + swapped[...].astype(F32)
    second[...] = joined.astype(BF16)
    direct[...] = image_part(weights, first, last, direct_step(), rows).astype(BF16)
    own[...] = image_part(weights, first, last, 0, rows)
    for slot, out in zip(sent_slots(parts)[1], kept):
        text_part(weights, images, slot, out)


def join_kernel(parts, kept, arrived, joined):
    end = at_end(parts)
    for at in range(0, kept.shape[0], CHUNK):
        chunk = slice(at, at + CHUNK)
        added = jnp.where(end, 0.0, arrived[chunk, :].astype(F32))
        joined[chunk, :] = (kept[chunk, :] + added).astype(BF16)


def final_kernel(n_always, n_end, parts, scale, raw, *refs):
    *refs, grad = refs
    always, ends, others = refs[:n_always], refs[n_always : n_always + n_end], refs[n_always + n_end :]
    factor = scale[0]
    end = at_end(parts)
    for at in range(0, raw.shape[0], CHUNK):
        chunk = slice(at, at + CHUNK)
        wide = raw[chunk, :].astype(F32)
        inverse = inverse_norm(wide)
        unit = wide * inverse
        total = sum(part[chunk, :].astype(F32) for part in always)
        if ends:
            at_ends = sum(part[chunk, :].astype(F32) for part in ends)
            total += jnp.where(end, at_ends, sum(part[chunk, :].astype(F32) for part in others))
        total = factor * total
        along = jnp.sum(unit * total, axis=-1, keepdims=True)
        grad[chunk, :] = (total - unit * along) * inverse


def call(kernel, outs, specs, args, scratch=()):
    return pl.pallas_call(
        kernel,
        out_shape=outs,
        in_specs=[pl.BlockSpec(memory_space=space) for space in specs],
        out_specs=jax.tree.map(lambda _: pl.BlockSpec(memory_space=VMEM), outs),
        scratch_shapes=list(scratch),
        compiler_params=pltpu.CompilerParams(vmem_limit_bytes=16 << 20),
    )(*args)


def is_line(parts):
    return parts == 4


def at_end(parts):
    quarter = lax.axis_index("rep")
    return (quarter == 0) | (quarter == parts - 1)


def near_slots(parts):
    if not is_line(parts):
        return list(range(1, parts - 1))
    first = jnp.where(at_end(parts), 1, 2)
    return [first, 3 - first]


def sent_slots(parts):
    if not is_line(parts):
        return list(range(1, parts)), [0]
    end = at_end(parts)
    return [jnp.where(end, 3, 1), jnp.where(end, 2, 3)], [0, jnp.where(end, 1, 2)]


def gathered_texts(text):
    parts = lax.axis_size("rep")
    if not is_line(parts):
        texts = [fetched(text, "rep", s) for s in range(1, parts)]
        return texts[:-1], texts[-1:]
    one = lax.ppermute(text, "rep", [(0, 2), (3, 1), (1, 0), (2, 3)])
    two = lax.ppermute(text, "rep", [(0, 1), (3, 2), (1, 3), (2, 0)])
    middle = middle_swapped(text)
    onward = lax.ppermute(one, "rep", [(1, 0), (2, 3), (0, 1), (3, 2)])
    return [one, two], [onward, middle]


def returned_texts(narrow, kept):
    parts = lax.axis_size("rep")
    if not is_line(parts):
        back = [returned(part, "rep", s) for s, part in enumerate(narrow, 1)]
        return [kept[0], *back], [], []
    early, late = narrow
    one = lax.ppermute(early, "rep", [(0, 1), (3, 2), (1, 0), (2, 3)])
    middle = middle_swapped(late)
    ends = lax.ppermute(late, "rep", [(0, 2), (3, 1), (1, 0), (2, 3)])
    joined = call(
        functools.partial(join_kernel, parts),
        jax.ShapeDtypeStruct(one.shape, BF16),
        [VMEM] * 2,
        (kept[1], one),
    )
    joined = lax.ppermute(joined, "rep", [(0, 1), (3, 2), (1, 3), (2, 0)])
    return [kept[0], joined], [one], [middle, ends]


def gathered_images(image):
    direct = lax.ppermute(image, "blk", [(b, a) for a, b in direct_pairs()])
    second = passed_along(image, "blk", -2)
    return direct, second, neighbour_swapped(second)


def known_row_tables(own):
    count = lax.axis_size("blk")
    tables = [own]
    if whole_axis_known(count):
        while sum(t.shape[0] for t in tables) < count * own.shape[0]:
            sent = jnp.concatenate(tables, axis=0)
            n = len(tables) - 1
            tables.append(fetched(sent, "blk", 2**n))
        return tables
    for n, (shift, known) in enumerate(doublings(STEPS - 1)):
        by_shift = {}
        for array, shifts in zip(tables, known_places(STEPS - 1)):
            for at, shifted in enumerate(shifts):
                by_shift[shifted] = array[at * 2 * STEPS : (at + 1) * 2 * STEPS]
        sent = jnp.concatenate([by_shift[t] for t in range(-known, known + 1)], axis=0)
        for sign in (1, -1):
            tables.append(passed_along(sent, "blk", -sign * shift))
    return tables


def on_device(image, text, positive, logit_scale):
    rows, width = image.shape
    parts = lax.axis_size("rep")
    height = table_rows(parts)
    shape = jax.ShapeDtypeStruct
    texts, text_last = gathered_texts(text)
    direct, second, other = gathered_images(image)
    own_image, own_text = call(
        own_kernel, [shape((rows, width), BF16)] * 2, [VMEM] * 2, (image, text)
    )
    split = (parts - 1) * rows
    img_tiles, first, txt_first, row_first, col_first = call(
        functools.partial(first_kernel, parts),
        (
            shape((STEPS * rows, width), BF16),
            shape((STEPS * rows, split), F32),
            shape((split, width), BF16),
            shape((2 * STEPS + 1, rows), F32),
            shape((3 * (parts - 1), rows), F32),
        ),
        [SMEM] + [VMEM] * (6 + len(texts)),
        (logit_scale, positive, own_image, direct, second, other, own_text, *texts),
    )
    last, txt_last, row_stats, col_stats, row_pos = call(
        functools.partial(last_kernel, parts),
        (
            shape((STEPS * rows, rows), F32),
            shape((rows, width), BF16),
            shape((2 * STEPS, rows), F32),
            shape((height, rows), F32),
            shape((1, rows), F32),
        ),
        [SMEM] + [VMEM] * (4 + len(text_last)),
        (logit_scale, positive, img_tiles, row_first, col_first, *text_last),
        [pltpu.VMEM((2 * STEPS + 1, rows), F32), pltpu.VMEM((3, rows), F32)],
    )
    col_tables = [col_stats]
    for n, count in enumerate(slot_counts(parts)[1:]):
        sent = jnp.concatenate(col_tables, axis=0)[: count * height]
        col_tables.append(fetched(sent, "rep", 2**n))
    row_tables = known_row_tables(row_stats)
    narrow_slots, kept_slots = sent_slots(parts)
    row_loss, col_loss, weights, other, *narrow = call(
        functools.partial(weights_kernel, parts, len(row_tables)),
        (
            shape((1, rows), F32),
            shape((1, rows), F32),
            shape((STEPS * rows, parts * rows), BF16),
            *[shape((rows, width), BF16) for _ in range(1 + len(narrow_slots))],
        ),
        [VMEM] * (7 + len(row_tables) + len(col_tables)),
        (
            positive,
            first,
            last,
            img_tiles,
            txt_first,
            txt_last,
            row_pos,
            *row_tables,
            *col_tables,
        ),
        [pltpu.VMEM((sum(t.shape[0] for t in row_tables), rows), F32)],
    )
    swapped = neighbour_swapped(other)
    own, direct, second, *kept = call(
        functools.partial(rest_kernel, parts),
        [shape((rows, width), t) for t in (F32, BF16, BF16, *[F32 for _ in kept_slots])],
        [VMEM] * 5,
        (weights, img_tiles, txt_first, txt_last, swapped),
    )
    img_sums = [own, lax.ppermute(direct, "blk", direct_pairs()), passed_along(second, "blk", 2)]
    txt_sums = returned_texts(narrow, kept)
    grads = []
    for raw, (always, ends, others) in ((image, (img_sums, [], [])), (text, txt_sums)):
        sums = [*always, *ends, *others]
        grads.append(
            call(
                functools.partial(final_kernel, len(always), len(ends), parts),
                shape((rows, width), F32),
                [SMEM] + [VMEM] * (1 + len(sums)),
                (logit_scale, raw, *sums),
            )
        )
    return (row_loss[0], col_loss[0], *grads)


def solution(mesh):
    placed = (P(("blk", "rep"), None), P(("blk", "rep"), None), P("blk", "rep"), P())

    return jax.shard_map(
        on_device,
        mesh=mesh,
        in_specs=placed,
        out_specs=(
            P(("blk", "rep")),
            P(("blk", "rep")),
            P(("blk", "rep"), None),
            P(("blk", "rep"), None),
        ),
        check_vma=False,
    )
```

```python
import functools

import jax
import jax.numpy as jnp
from jax import lax
from jax.experimental import pallas as pl
from jax.experimental.pallas import tpu as pltpu
from jax.sharding import PartitionSpec as P

STEPS = 4
CHUNK = 16
F32 = jnp.float32
BF16 = jnp.bfloat16
VMEM = pltpu.VMEM
SMEM = pltpu.SMEM


def power_of_two(count):
    return count & (count - 1) == 0


def place(own, slot, count):
    return own ^ slot if power_of_two(count) else (own + slot) % count


def slot_at(slot, partner, count):
    return slot ^ partner if power_of_two(count) else (slot - partner) % count


def fetched(array, axis, slot):
    count = lax.axis_size(axis)
    return lax.ppermute(array, axis, [(place(i, slot, count), i) for i in range(count)])


def returned(array, axis, slot):
    count = lax.axis_size(axis)
    return lax.ppermute(array, axis, [(i, place(i, slot, count)) for i in range(count)])


def passed_along(array, axis, by):
    count = lax.axis_size(axis)
    return lax.ppermute(array, axis, [(i, (i + by) % count) for i in range(count)])


def middle_swapped(array):
    parts, blocks = lax.axis_size("rep"), lax.axis_size("blk")
    pairs = [
        (b * parts + r, b * parts + parts - 1 - r if 0 < r < parts - 1 else (b ^ 1) * parts + r)
        for b in range(blocks)
        for r in range(parts)
    ]
    return lax.ppermute(array, ("blk", "rep"), pairs)


def neighbour_swapped(array):
    count = lax.axis_size("blk")
    return lax.ppermute(array, "blk", [(i, i ^ 1) for i in range(count)])


def direct_pairs():
    count = lax.axis_size("blk")
    return [(i, (i + (3 if i % 2 else 1)) % count) for i in range(count)]


def direct_step():
    return jnp.where(lax.axis_index("blk") % 2 == 0, 1, 3)


def table_rows(parts):
    return -(-3 * parts // 8) * 8


def doublings(reach):
    known, rounds = 0, []
    while known < reach:
        shift = min(2 * known + 1, reach - known)
        rounds.append((shift, known))
        known += shift
    return rounds


def known_places(reach):
    held = [[0]]
    for shift, known in doublings(reach):
        for centre in (shift, -shift):
            held.append(list(range(centre - known, centre + known + 1)))
    return held


def whole_axis_known(count):
    return power_of_two(count) and count <= 2 * STEPS


def slot_counts(parts):
    counts = [1]
    while sum(counts) < parts:
        counts.append(min(sum(counts), parts - sum(counts)))
    return counts


def inverse_norm(wide):
    return lax.rsqrt(jnp.sum(wide * wide, axis=-1, keepdims=True) + 1e-06)


def store_units(raw, out, base):
    for at in range(0, raw.shape[0], CHUNK):
        wide = raw[at : at + CHUNK, :].astype(F32)
        here = pl.multiple_of(base + at, CHUNK)
        out[pl.ds(here, CHUNK), :] = (wide * inverse_norm(wide)).astype(BF16)


def own_kernel(image, text, img_out, txt_out):
    store_units(image, img_out, 0)
    store_units(text, txt_out, 0)


def diagonal(rows):
    return lax.broadcasted_iota(jnp.int32, (rows, rows), 0) == lax.broadcasted_iota(
        jnp.int32, (rows, rows), 1
    )


def to_lanes(column, eye):
    return jnp.sum(jnp.where(eye, column, 0.0), axis=0, keepdims=True)


def to_column(lanes, eye):
    return jnp.sum(jnp.where(eye, lanes, 0.0), axis=1, keepdims=True)


def onehot_of(positive, eye, parts, rows):
    wanted = to_column(positive.astype(F32), eye)
    lane = lax.broadcasted_iota(jnp.int32, (rows, rows), 1)
    quarter = lax.axis_index("rep")
    return [wanted == (lane + place(quarter, s, parts) * rows).astype(F32) for s in range(parts)]


def scores_kernel(parts, slots, factor, positive, images, scores, txt_out, row_out, col_out):
    rows = positive.shape[1]
    eye = diagonal(rows)
    wanted = to_column(positive.astype(F32), eye)
    lane = lax.broadcasted_iota(jnp.int32, (rows, rows), 1)
    quarter = lax.axis_index("rep")
    scores[...] = factor * lax.dot_general(
        images[...], txt_out[...], (((1,), (1,)), ((), ())), preferred_element_type=F32
    )
    peaks, sums = [], []
    for k in range(STEPS):
        tile = scores[k * rows : (k + 1) * rows, :]
        peak = jnp.max(tile, axis=1, keepdims=True)
        peaks.append(to_lanes(peak, eye))
        sums.append(to_lanes(jnp.sum(jnp.exp(tile - peak), axis=1, keepdims=True), eye))
    found = jnp.zeros((rows, 1), F32)
    col_peaks, col_sums, picked = [], [], []
    for n, s in enumerate(slots):
        tile = scores[:, n * rows : (n + 1) * rows]
        peak = jnp.max(tile, axis=0, keepdims=True)
        col_peaks.append(peak)
        col_sums.append(jnp.sum(jnp.exp(tile - peak), axis=0, keepdims=True))
        match = wanted == (lane + place(quarter, s, parts) * rows).astype(F32)
        chosen = jnp.where(match, tile[:rows, :], 0.0)
        picked.append(jnp.sum(chosen, axis=0, keepdims=True))
        found = found + jnp.sum(chosen, axis=1, keepdims=True)
    row_out[...] = jnp.concatenate(peaks + sums + [to_lanes(found, eye)], axis=0)
    col_out[...] = jnp.concatenate(col_peaks + col_sums + picked, axis=0)


def first_kernel(parts, scale, positive, *refs):
    own_image, direct, second, other, own_text = refs[:5]
    texts = refs[5 : 5 + parts - 2]
    img_out, scores, txt_out, *stats = refs[5 + parts - 2 :]
    rows = own_image.shape[0]
    step = direct_step()
    img_out[:rows, :] = own_image[...]
    store_units(direct, img_out, step * rows)
    store_units(second, img_out, 2 * rows)
    store_units(other, img_out, (STEPS - step) * rows)
    txt_out[:rows, :] = own_text[...]
    for slot, text in zip(near_slots(parts), texts):
        store_units(text, txt_out, slot * rows)
    slots = range(parts - 1)
    scores_kernel(parts, slots, scale[0], positive[...], img_out, scores, txt_out, *stats)


def last_kernel(parts, scale, positive, images, row_first, col_first, *refs):
    *texts, scores, txt_out, row_stats, col_stats, row_pos, row_last, col_last = refs
    if len(texts) == 1:
        store_units(texts[0], txt_out, 0)
    else:
        end = at_end(parts)
        pl.when(end)(lambda: store_units(texts[0], txt_out, 0))
        pl.when(jnp.logical_not(end))(lambda: store_units(texts[1], txt_out, 0))
    slots = [parts - 1]
    scores_kernel(
        parts, slots, scale[0], positive[...], images, scores, txt_out, row_last, col_last
    )
    peaks = jnp.maximum(row_first[:STEPS, :], row_last[:STEPS, :])
    sums = sum(
        t[STEPS : 2 * STEPS, :] * jnp.exp(t[:STEPS, :] - peaks) for t in (row_first, row_last)
    )
    row_stats[...] = jnp.concatenate([peaks, sums], axis=0)
    row_pos[...] = row_first[2 * STEPS :, :] + row_last[2 * STEPS :, :]
    tables = []
    for which in range(3):
        tables += [col_first[which * (parts - 1) : (which + 1) * (parts - 1), :]]
        tables += [col_last[which : which + 1, :]]
    blank = jnp.zeros((col_stats.shape[0] - 3 * parts, col_last.shape[1]), F32)
    col_stats[...] = jnp.concatenate(tables + [blank] * (blank.shape[0] > 0), axis=0)


def merged(pairs):
    peak = functools.reduce(jnp.maximum, [p for p, _ in pairs])
    return peak + jnp.log(sum(s * jnp.exp(p - peak) for p, s in pairs))


def row_table_lookup(refs, tables):
    height = 2 * STEPS
    at = 0
    for ref in refs:
        tables[at : at + ref.shape[0], :] = ref[...]
        at += ref.shape[0]
    if whole_axis_known(lax.axis_size("blk")):
        count = lax.axis_size("blk")
        own = lax.axis_index("blk")

        def lookup(shift):
            slot = own ^ ((own + shift + count) % count)
            return tables[pl.ds(pl.multiple_of(slot * height, height), height), :]

        return lookup
    order = [shift for held in known_places(STEPS - 1) for shift in held]
    return lambda shift: tables[pl.ds(order.index(shift) * height, height), :]


def weights_kernel(parts, n_rows, positive, first, last, images, txt_first, txt_last, *refs):
    row_refs, refs = refs[:n_rows], refs[n_rows:]
    held = slot_counts(parts)
    col_refs, refs = refs[: len(held)], refs[len(held) :]
    row_out, col_out, col_picked, weights, other, *narrow, row_scratch = refs
    rows = positive.shape[1]
    eye = diagonal(rows)
    onehot = onehot_of(positive[...], eye, parts, rows)
    row_table = row_table_lookup(row_refs, row_scratch)
    row_tables = {shift: row_table(shift) for shift in range(1 - STEPS, STEPS)}
    height = table_rows(parts)
    col_tables = []
    for ref, count in zip(col_refs, held):
        col_tables += [ref[n * height : (n + 1) * height, :] for n in range(count)]

    def row_pair(shift, k):
        table, at = row_tables[shift], k - shift
        return table[at : at + 1, :], table[STEPS + at : STEPS + at + 1, :]

    row_lse = []
    for k in range(STEPS):
        lse = merged([row_pair(t, k) for t in range(1 - STEPS, STEPS) if 0 <= k - t < STEPS])
        if k == 0:
            row_out[...] = lse
        row_lse.append(to_column(lse, eye))
    col_lse = []
    for s in range(parts):
        at = [(col_tables[t], slot_at(s, t, parts)) for t in range(parts)]
        lse = merged([(c[q : q + 1, :], c[parts + q : parts + q + 1, :]) for c, q in at])
        if s == 0:
            col_out[...] = lse
            col_picked[...] = sum(c[2 * parts + q : 2 * parts + q + 1, :] for c, q in at)
        col_lse.append(lse)
    for s in range(parts):
        source, base = (first, s * rows) if s < parts - 1 else (last, 0)
        for k in range(STEPS):
            tile = source[k * rows : (k + 1) * rows, base : base + rows]
            weight = 0.5 * (jnp.exp(tile - row_lse[k]) + jnp.exp(tile - col_lse[s]))
            if k == 0:
                weight = weight - onehot[s].astype(F32)
            weights[k * rows : (k + 1) * rows, s * rows : (s + 1) * rows] = weight.astype(BF16)
    for slot, out in zip(sent_slots(parts)[0], narrow):
        text_part(weights, images, slot, out)
    other[...] = image_part(weights, txt_first, txt_last, STEPS - direct_step(), rows).astype(BF16)


def text_part(weights, images, slot, out):
    rows = out.shape[0]
    strip = pl.ds(pl.multiple_of(slot * rows, rows), rows)
    part = lax.dot_general(
        weights[:, strip], images[...], (((0,), (0,)), ((), ())), preferred_element_type=F32
    )
    out[...] = part.astype(out.dtype)


def image_part(weights, first, last, k, rows):
    strip = pl.ds(pl.multiple_of(k * rows, rows), rows)
    split = first.shape[0]
    part = jnp.dot(weights[strip, :split], first[...], preferred_element_type=F32)
    return part + jnp.dot(weights[strip, split:], last[...], preferred_element_type=F32)


def passed_kernel(weights, first, last, swapped, direct, second):
    rows = second.shape[0]
    joined = image_part(weights, first, last, 2, rows) + swapped[...].astype(F32)
    second[...] = joined.astype(BF16)
    direct[...] = image_part(weights, first, last, direct_step(), rows).astype(BF16)


def rest_kernel(parts, weights, images, first, last, own, *kept):
    for slot, out in reversed(list(zip(sent_slots(parts)[1], kept))):
        text_part(weights, images, slot, out)
    own[...] = image_part(weights, first, last, 0, own.shape[0])


def join_kernel(parts, kept, arrived, joined):
    end = at_end(parts)
    for at in range(0, kept.shape[0], CHUNK):
        chunk = slice(at, at + CHUNK)
        added = jnp.where(end, 0.0, arrived[chunk, :].astype(F32))
        joined[chunk, :] = (kept[chunk, :] + added).astype(BF16)


def final_kernel(n_always, n_end, parts, scale, raw, *refs):
    *refs, grad = refs
    always, ends, others = refs[:n_always], refs[n_always : n_always + n_end], refs[n_always + n_end :]
    factor = scale[0]
    end = at_end(parts)
    for at in range(0, raw.shape[0], CHUNK):
        chunk = slice(at, at + CHUNK)
        wide = raw[chunk, :].astype(F32)
        inverse = inverse_norm(wide)
        unit = wide * inverse
        total = sum(part[chunk, :].astype(F32) for part in always)
        if ends:
            at_ends = sum(part[chunk, :].astype(F32) for part in ends)
            total += jnp.where(end, at_ends, sum(part[chunk, :].astype(F32) for part in others))
        total = factor * total
        along = jnp.sum(unit * total, axis=-1, keepdims=True)
        grad[chunk, :] = (total - unit * along) * inverse


def call(kernel, outs, specs, args, scratch=()):
    return pl.pallas_call(
        kernel,
        out_shape=outs,
        in_specs=[pl.BlockSpec(memory_space=space) for space in specs],
        out_specs=jax.tree.map(lambda _: pl.BlockSpec(memory_space=VMEM), outs),
        scratch_shapes=list(scratch),
        compiler_params=pltpu.CompilerParams(vmem_limit_bytes=16 << 20),
    )(*args)


def is_line(parts):
    return parts == 4


def at_end(parts):
    quarter = lax.axis_index("rep")
    return (quarter == 0) | (quarter == parts - 1)


def near_slots(parts):
    if not is_line(parts):
        return list(range(1, parts - 1))
    first = jnp.where(at_end(parts), 1, 2)
    return [first, 3 - first]


def sent_slots(parts):
    if not is_line(parts):
        return list(range(1, parts)), [0]
    end = at_end(parts)
    return [jnp.where(end, 3, 1), jnp.where(end, 2, 3)], [0, jnp.where(end, 1, 2)]


def gathered_texts(text):
    parts = lax.axis_size("rep")
    if not is_line(parts):
        texts = [fetched(text, "rep", s) for s in range(1, parts)]
        return texts[:-1], texts[-1:]
    one = lax.ppermute(text, "rep", [(0, 2), (3, 1), (1, 0), (2, 3)])
    two = lax.ppermute(text, "rep", [(0, 1), (3, 2), (1, 3), (2, 0)])
    middle = middle_swapped(text)
    onward = lax.ppermute(one, "rep", [(1, 0), (2, 3), (0, 1), (3, 2)])
    return [one, two], [onward, middle]


def returned_texts(narrow, kept):
    parts = lax.axis_size("rep")
    if not is_line(parts):
        back = [returned(part, "rep", s) for s, part in enumerate(narrow, 1)]
        return [kept[0], *back], [], []
    early, late = narrow
    one = lax.ppermute(early, "rep", [(0, 1), (3, 2), (1, 0), (2, 3)])
    middle = middle_swapped(late)
    ends = lax.ppermute(late, "rep", [(0, 2), (3, 1), (1, 0), (2, 3)])
    joined = call(
        functools.partial(join_kernel, parts),
        jax.ShapeDtypeStruct(one.shape, BF16),
        [VMEM] * 2,
        (kept[1], one),
    )
    joined = lax.ppermute(joined, "rep", [(0, 1), (3, 2), (1, 3), (2, 0)])
    return [kept[0], joined], [one], [middle, ends]


def gathered_images(image):
    direct = lax.ppermute(image, "blk", [(b, a) for a, b in direct_pairs()])
    second = passed_along(image, "blk", -2)
    return direct, second, neighbour_swapped(second)


def known_row_tables(own):
    count = lax.axis_size("blk")
    tables = [own]
    if whole_axis_known(count):
        while sum(t.shape[0] for t in tables) < count * own.shape[0]:
            sent = jnp.concatenate(tables, axis=0)
            n = len(tables) - 1
            tables.append(fetched(sent, "blk", 2**n))
        return tables
    for n, (shift, known) in enumerate(doublings(STEPS - 1)):
        by_shift = {}
        for array, shifts in zip(tables, known_places(STEPS - 1)):
            for at, shifted in enumerate(shifts):
                by_shift[shifted] = array[at * 2 * STEPS : (at + 1) * 2 * STEPS]
        sent = jnp.concatenate([by_shift[t] for t in range(-known, known + 1)], axis=0)
        for sign in (1, -1):
            tables.append(passed_along(sent, "blk", -sign * shift))
    return tables


def on_device(image, text, positive, logit_scale):
    rows, width = image.shape
    parts = lax.axis_size("rep")
    height = table_rows(parts)
    shape = jax.ShapeDtypeStruct
    texts, text_last = gathered_texts(text)
    direct, second, other = gathered_images(image)
    own_image, own_text = call(
        own_kernel, [shape((rows, width), BF16)] * 2, [VMEM] * 2, (image, text)
    )
    split = (parts - 1) * rows
    img_tiles, first, txt_first, row_first, col_first = call(
        functools.partial(first_kernel, parts),
        (
            shape((STEPS * rows, width), BF16),
            shape((STEPS * rows, split), F32),
            shape((split, width), BF16),
            shape((2 * STEPS + 1, rows), F32),
            shape((3 * (parts - 1), rows), F32),
        ),
        [SMEM] + [VMEM] * (6 + len(texts)),
        (logit_scale, positive, own_image, direct, second, other, own_text, *texts),
    )
    last, txt_last, row_stats, col_stats, row_pos = call(
        functools.partial(last_kernel, parts),
        (
            shape((STEPS * rows, rows), F32),
            shape((rows, width), BF16),
            shape((2 * STEPS, rows), F32),
            shape((height, rows), F32),
            shape((1, rows), F32),
        ),
        [SMEM] + [VMEM] * (4 + len(text_last)),
        (logit_scale, positive, img_tiles, row_first, col_first, *text_last),
        [pltpu.VMEM((2 * STEPS + 1, rows), F32), pltpu.VMEM((3, rows), F32)],
    )
    col_tables = [col_stats]
    for n, count in enumerate(slot_counts(parts)[1:]):
        sent = jnp.concatenate(col_tables, axis=0)[: count * height]
        col_tables.append(fetched(sent, "rep", 2**n))
    row_tables = known_row_tables(row_stats)
    narrow_slots, kept_slots = sent_slots(parts)
    row_lse, col_lse, col_pos, weights, other, *narrow = call(
        functools.partial(weights_kernel, parts, len(row_tables)),
        (
            *[shape((1, rows), F32)] * 3,
            shape((STEPS * rows, parts * rows), BF16),
            *[shape((rows, width), BF16) for _ in range(1 + len(narrow_slots))],
        ),
        [VMEM] * (6 + len(row_tables) + len(col_tables)),
        (
            positive,
            first,
            last,
            img_tiles,
            txt_first,
            txt_last,
            *row_tables,
            *col_tables,
        ),
        [pltpu.VMEM((sum(t.shape[0] for t in row_tables), rows), F32)],
    )
    swapped = neighbour_swapped(other)
    direct, second = call(
        passed_kernel,
        [shape((rows, width), BF16)] * 2,
        [VMEM] * 4,
        (weights, txt_first, txt_last, swapped),
    )
    own, *kept = call(
        functools.partial(rest_kernel, parts),
        [shape((rows, width), F32) for _ in range(1 + len(kept_slots))],
        [VMEM] * 4,
        (weights, img_tiles, txt_first, txt_last),
    )
    img_sums = [own, lax.ppermute(direct, "blk", direct_pairs()), passed_along(second, "blk", 2)]
    txt_sums = returned_texts(narrow, kept)
    grads = []
    for raw, (always, ends, others) in ((image, (img_sums, [], [])), (text, txt_sums)):
        sums = [*always, *ends, *others]
        grads.append(
            call(
                functools.partial(final_kernel, len(always), len(ends), parts),
                shape((rows, width), F32),
                [SMEM] + [VMEM] * (1 + len(sums)),
                (logit_scale, raw, *sums),
            )
        )
    row_loss = row_lse[0] - row_pos[0]
    col_loss = col_lse[0] - col_pos[0]
    return (row_loss, col_loss, *grads)


def solution(mesh):
    placed = (P(("blk", "rep"), None), P(("blk", "rep"), None), P("blk", "rep"), P())

    return jax.shard_map(
        on_device,
        mesh=mesh,
        in_specs=placed,
        out_specs=(
            P(("blk", "rep")),
            P(("blk", "rep")),
            P(("blk", "rep"), None),
            P(("blk", "rep"), None),
        ),
        check_vma=False,
    )
```

```python
import functools

import jax
import jax.numpy as jnp
from jax import lax
from jax.experimental import pallas as pl
from jax.experimental.pallas import tpu as pltpu
from jax.sharding import PartitionSpec as P

STEPS = 4
CHUNK = 16
F32 = jnp.float32
BF16 = jnp.bfloat16
VMEM = pltpu.VMEM
SMEM = pltpu.SMEM


def power_of_two(count):
    return count & (count - 1) == 0


def place(own, slot, count):
    return own ^ slot if power_of_two(count) else (own + slot) % count


def slot_at(slot, partner, count):
    return slot ^ partner if power_of_two(count) else (slot - partner) % count


def fetched(array, axis, slot):
    count = lax.axis_size(axis)
    return lax.ppermute(array, axis, [(place(i, slot, count), i) for i in range(count)])


def returned(array, axis, slot):
    count = lax.axis_size(axis)
    return lax.ppermute(array, axis, [(i, place(i, slot, count)) for i in range(count)])


def passed_along(array, axis, by):
    count = lax.axis_size(axis)
    return lax.ppermute(array, axis, [(i, (i + by) % count) for i in range(count)])


def middle_swapped(array):
    parts, blocks = lax.axis_size("rep"), lax.axis_size("blk")
    pairs = [
        (b * parts + r, b * parts + parts - 1 - r if 0 < r < parts - 1 else (b ^ 1) * parts + r)
        for b in range(blocks)
        for r in range(parts)
    ]
    return lax.ppermute(array, ("blk", "rep"), pairs)


def neighbour_swapped(array):
    count = lax.axis_size("blk")
    return lax.ppermute(array, "blk", [(i, i ^ 1) for i in range(count)])


def direct_pairs():
    count = lax.axis_size("blk")
    return [(i, (i + (3 if i % 2 else 1)) % count) for i in range(count)]


def direct_step():
    return jnp.where(lax.axis_index("blk") % 2 == 0, 1, 3)


def table_rows(parts):
    return -(-3 * parts // 8) * 8


def doublings(reach):
    known, rounds = 0, []
    while known < reach:
        shift = min(2 * known + 1, reach - known)
        rounds.append((shift, known))
        known += shift
    return rounds


def known_places(reach):
    held = [[0]]
    for shift, known in doublings(reach):
        for centre in (shift, -shift):
            held.append(list(range(centre - known, centre + known + 1)))
    return held


def whole_axis_known(count):
    return power_of_two(count) and count <= 2 * STEPS


def slot_counts(parts):
    counts = [1]
    while sum(counts) < parts:
        counts.append(min(sum(counts), parts - sum(counts)))
    return counts


def inverse_norm(wide):
    return lax.rsqrt(jnp.sum(wide * wide, axis=-1, keepdims=True) + 1e-06)


def store_units(raw, out, base):
    for at in range(0, raw.shape[0], CHUNK):
        wide = raw[at : at + CHUNK, :].astype(F32)
        here = pl.multiple_of(base + at, CHUNK)
        out[pl.ds(here, CHUNK), :] = (wide * inverse_norm(wide)).astype(BF16)


def own_kernel(image, text, img_out, txt_out):
    store_units(image, img_out, 0)
    store_units(text, txt_out, 0)


def diagonal(rows):
    return lax.broadcasted_iota(jnp.int32, (rows, rows), 0) == lax.broadcasted_iota(
        jnp.int32, (rows, rows), 1
    )


def to_lanes(column, eye):
    return jnp.sum(jnp.where(eye, column, 0.0), axis=0, keepdims=True)


def to_column(lanes, eye):
    return jnp.sum(jnp.where(eye, lanes, 0.0), axis=1, keepdims=True)


def onehot_of(positive, eye, parts, rows):
    wanted = to_column(positive.astype(F32), eye)
    lane = lax.broadcasted_iota(jnp.int32, (rows, rows), 1)
    quarter = lax.axis_index("rep")
    return [
        wanted == (lane + place(quarter, slot_at_position(s, parts), parts) * rows).astype(F32)
        for s in range(parts)
    ]


def scores_kernel(parts, slots, factor, positive, images, scores, txt_out, row_out, col_out):
    rows = positive.shape[1]
    eye = diagonal(rows)
    wanted = to_column(positive.astype(F32), eye)
    lane = lax.broadcasted_iota(jnp.int32, (rows, rows), 1)
    quarter = lax.axis_index("rep")
    scores[...] = factor * lax.dot_general(
        images[...], txt_out[...], (((1,), (1,)), ((), ())), preferred_element_type=F32
    )
    peaks, sums = [], []
    for k in range(STEPS):
        tile = scores[k * rows : (k + 1) * rows, :]
        peak = jnp.max(tile, axis=1, keepdims=True)
        peaks.append(to_lanes(peak, eye))
        sums.append(to_lanes(jnp.sum(jnp.exp(tile - peak), axis=1, keepdims=True), eye))
    found = jnp.zeros((rows, 1), F32)
    col_peaks, col_sums, picked = [], [], []
    for n, s in enumerate(slots):
        tile = scores[:, n * rows : (n + 1) * rows]
        peak = jnp.max(tile, axis=0, keepdims=True)
        col_peaks.append(peak)
        col_sums.append(jnp.sum(jnp.exp(tile - peak), axis=0, keepdims=True))
        column = lane + place(quarter, slot_at_position(s, parts), parts) * rows
        match = wanted == column.astype(F32)
        chosen = jnp.where(match, tile[:rows, :], 0.0)
        picked.append(jnp.sum(chosen, axis=0, keepdims=True))
        found = found + jnp.sum(chosen, axis=1, keepdims=True)
    row_out[...] = jnp.concatenate(peaks + sums + [to_lanes(found, eye)], axis=0)
    col_out[...] = jnp.concatenate(col_peaks + col_sums + picked, axis=0)


def first_kernel(parts, scale, positive, *refs):
    own_image, direct, second, other, own_text = refs[:5]
    texts = refs[5 : 5 + parts - 2]
    img_out, scores, txt_out, *stats = refs[5 + parts - 2 :]
    rows = own_image.shape[0]
    step = direct_step()
    img_out[:rows, :] = own_image[...]
    store_units(direct, img_out, step * rows)
    store_units(second, img_out, 2 * rows)
    store_units(other, img_out, (STEPS - step) * rows)
    txt_out[:rows, :] = own_text[...]
    for n, text in enumerate(texts, 1):
        store_units(text, txt_out, n * rows)
    slots = range(parts - 1)
    scores_kernel(parts, slots, scale[0], positive[...], img_out, scores, txt_out, *stats)


def last_kernel(parts, scale, positive, images, row_first, col_first, *refs):
    *texts, scores, txt_out, row_stats, col_stats, row_pos, row_last, col_last = refs
    if len(texts) == 1:
        store_units(texts[0], txt_out, 0)
    else:
        end = at_end(parts)
        pl.when(end)(lambda: store_units(texts[0], txt_out, 0))
        pl.when(jnp.logical_not(end))(lambda: store_units(texts[1], txt_out, 0))
    slots = [parts - 1]
    scores_kernel(
        parts, slots, scale[0], positive[...], images, scores, txt_out, row_last, col_last
    )
    peaks = jnp.maximum(row_first[:STEPS, :], row_last[:STEPS, :])
    sums = sum(
        t[STEPS : 2 * STEPS, :] * jnp.exp(t[:STEPS, :] - peaks) for t in (row_first, row_last)
    )
    row_stats[...] = jnp.concatenate([peaks, sums], axis=0)
    row_pos[...] = row_first[2 * STEPS :, :] + row_last[2 * STEPS :, :]
    tables = []
    for which in range(3):
        at = which * (parts - 1)
        near = [col_first[at + n : at + n + 1, :] for n in range(parts - 1)]
        tables += reordered([*near, col_last[which : which + 1, :]], parts)
    blank = jnp.zeros((col_stats.shape[0] - 3 * parts, col_last.shape[1]), F32)
    col_stats[...] = jnp.concatenate(tables + [blank] * (blank.shape[0] > 0), axis=0)


def merged(pairs):
    peak = functools.reduce(jnp.maximum, [p for p, _ in pairs])
    return peak + jnp.log(sum(s * jnp.exp(p - peak) for p, s in pairs))


def row_table_lookup(refs, tables):
    height = 2 * STEPS
    at = 0
    for ref in refs:
        tables[at : at + ref.shape[0], :] = ref[...]
        at += ref.shape[0]
    if whole_axis_known(lax.axis_size("blk")):
        count = lax.axis_size("blk")
        own = lax.axis_index("blk")

        def lookup(shift):
            slot = own ^ ((own + shift + count) % count)
            return tables[pl.ds(pl.multiple_of(slot * height, height), height), :]

        return lookup
    order = [shift for held in known_places(STEPS - 1) for shift in held]
    return lambda shift: tables[pl.ds(order.index(shift) * height, height), :]


def weights_kernel(parts, n_rows, positive, first, last, images, txt_first, txt_last, *refs):
    row_refs, refs = refs[:n_rows], refs[n_rows:]
    held = slot_counts(parts)
    col_refs, refs = refs[: len(held)], refs[len(held) :]
    row_out, col_out, col_picked, weights, other, *narrow, row_scratch = refs
    rows = positive.shape[1]
    eye = diagonal(rows)
    onehot = onehot_of(positive[...], eye, parts, rows)
    row_table = row_table_lookup(row_refs, row_scratch)
    row_tables = {shift: row_table(shift) for shift in range(1 - STEPS, STEPS)}
    height = table_rows(parts)
    col_tables = []
    for ref, count in zip(col_refs, held):
        col_tables += [ref[n * height : (n + 1) * height, :] for n in range(count)]

    def row_pair(shift, k):
        table, at = row_tables[shift], k - shift
        return table[at : at + 1, :], table[STEPS + at : STEPS + at + 1, :]

    row_lse = []
    for k in range(STEPS):
        lse = merged([row_pair(t, k) for t in range(1 - STEPS, STEPS) if 0 <= k - t < STEPS])
        if k == 0:
            row_out[...] = lse
        row_lse.append(to_column(lse, eye))
    col_lse = []
    for s in range(parts):
        at = [(col_tables[t], slot_at(s, t, parts)) for t in range(parts)]
        lse = merged([(c[q : q + 1, :], c[parts + q : parts + q + 1, :]) for c, q in at])
        if s == 0:
            col_out[...] = lse
            col_picked[...] = sum(c[2 * parts + q : 2 * parts + q + 1, :] for c, q in at)
        col_lse.append(lse)
    col_lse = reordered(col_lse, parts)

    def weigh(s):
        source, base = (first, s * rows) if s < parts - 1 else (last, 0)
        for k in range(STEPS):
            tile = source[k * rows : (k + 1) * rows, base : base + rows]
            weight = 0.5 * (jnp.exp(tile - row_lse[k]) + jnp.exp(tile - col_lse[s]))
            if k == 0:
                weight = weight - onehot[s].astype(F32)
            weights[k * rows : (k + 1) * rows, s * rows : (s + 1) * rows] = weight.astype(BF16)

    if is_line(parts):
        early, late = narrow
        weigh(2)
        weigh(3)
        end = at_end(parts)
        part = text_parts(weights, images, 2, 4, rows)
        one, other_one = part[:rows], part[rows:]
        early[...] = jnp.where(end, other_one, one).astype(BF16)
        late[...] = jnp.where(end, one, other_one).astype(BF16)
        weigh(0)
        weigh(1)
    else:
        for s in range(parts):
            weigh(s)
        for s, out in enumerate(narrow, 1):
            out[...] = text_parts(weights, images, s, s + 1, rows).astype(BF16)
    other[...] = image_part(weights, txt_first, txt_last, STEPS - direct_step(), rows).astype(BF16)


def text_parts(weights, images, begin, stop, rows):
    strip = slice(begin * rows, stop * rows)
    return lax.dot_general(
        weights[:, strip], images[...], (((0,), (0,)), ((), ())), preferred_element_type=F32
    )


def image_part(weights, first, last, k, rows):
    strip = pl.ds(pl.multiple_of(k * rows, rows), rows)
    split = first.shape[0]
    part = jnp.dot(weights[strip, :split], first[...], preferred_element_type=F32)
    return part + jnp.dot(weights[strip, split:], last[...], preferred_element_type=F32)


def passed_kernel(weights, first, last, swapped, direct, second):
    rows = second.shape[0]
    joined = image_part(weights, first, last, 2, rows) + swapped[...].astype(F32)
    second[...] = joined.astype(BF16)
    direct[...] = image_part(weights, first, last, direct_step(), rows).astype(BF16)


def rest_kernel(weights, images, first, last, own, *kept):
    rows = own.shape[0]
    part = text_parts(weights, images, 0, len(kept), rows)
    for n, out in enumerate(kept):
        out[...] = part[n * rows : (n + 1) * rows]
    own[...] = image_part(weights, first, last, 0, own.shape[0])


def join_kernel(parts, kept, arrived, joined):
    end = at_end(parts)
    for at in range(0, kept.shape[0], CHUNK):
        chunk = slice(at, at + CHUNK)
        added = jnp.where(end, 0.0, arrived[chunk, :].astype(F32))
        joined[chunk, :] = (kept[chunk, :] + added).astype(BF16)


def final_kernel(n_always, n_end, parts, scale, raw, *refs):
    *refs, grad = refs
    always, ends, others = refs[:n_always], refs[n_always : n_always + n_end], refs[n_always + n_end :]
    factor = scale[0]
    end = at_end(parts)
    for at in range(0, raw.shape[0], CHUNK):
        chunk = slice(at, at + CHUNK)
        wide = raw[chunk, :].astype(F32)
        inverse = inverse_norm(wide)
        unit = wide * inverse
        total = sum(part[chunk, :].astype(F32) for part in always)
        if ends:
            at_ends = sum(part[chunk, :].astype(F32) for part in ends)
            total += jnp.where(end, at_ends, sum(part[chunk, :].astype(F32) for part in others))
        total = factor * total
        along = jnp.sum(unit * total, axis=-1, keepdims=True)
        grad[chunk, :] = (total - unit * along) * inverse


def call(kernel, outs, specs, args, scratch=()):
    return pl.pallas_call(
        kernel,
        out_shape=outs,
        in_specs=[pl.BlockSpec(memory_space=space) for space in specs],
        out_specs=jax.tree.map(lambda _: pl.BlockSpec(memory_space=VMEM), outs),
        scratch_shapes=list(scratch),
        compiler_params=pltpu.CompilerParams(vmem_limit_bytes=16 << 20),
    )(*args)


def is_line(parts):
    return parts == 4


def at_end(parts):
    quarter = lax.axis_index("rep")
    return (quarter == 0) | (quarter == parts - 1)


def slot_at_position(position, parts):
    if is_line(parts) and position in (1, 2):
        return jnp.where(at_end(parts), position, 3 - position)
    return position


def reordered(rows, parts):
    if not is_line(parts):
        return rows
    end = at_end(parts)
    return [rows[0], jnp.where(end, rows[1], rows[2]), jnp.where(end, rows[2], rows[1]), rows[3]]


def gathered_texts(text):
    parts = lax.axis_size("rep")
    if not is_line(parts):
        texts = [fetched(text, "rep", s) for s in range(1, parts)]
        return texts[:-1], texts[-1:]
    one = lax.ppermute(text, "rep", [(0, 2), (3, 1), (1, 0), (2, 3)])
    two = lax.ppermute(text, "rep", [(0, 1), (3, 2), (1, 3), (2, 0)])
    middle = middle_swapped(text)
    onward = lax.ppermute(one, "rep", [(1, 0), (2, 3), (0, 1), (3, 2)])
    return [one, two], [onward, middle]


def returned_texts(narrow, kept):
    parts = lax.axis_size("rep")
    if not is_line(parts):
        back = [returned(part, "rep", s) for s, part in enumerate(narrow, 1)]
        return [kept[0], *back], [], []
    early, late = narrow
    one = lax.ppermute(early, "rep", [(0, 1), (3, 2), (1, 0), (2, 3)])
    middle = middle_swapped(late)
    ends = lax.ppermute(late, "rep", [(0, 2), (3, 1), (1, 0), (2, 3)])
    joined = call(
        functools.partial(join_kernel, parts),
        jax.ShapeDtypeStruct(one.shape, BF16),
        [VMEM] * 2,
        (kept[1], one),
    )
    joined = lax.ppermute(joined, "rep", [(0, 1), (3, 2), (1, 3), (2, 0)])
    return [kept[0], joined], [one], [middle, ends]


def gathered_images(image):
    direct = lax.ppermute(image, "blk", [(b, a) for a, b in direct_pairs()])
    second = passed_along(image, "blk", -2)
    return direct, second, neighbour_swapped(second)


def known_row_tables(own):
    count = lax.axis_size("blk")
    tables = [own]
    if whole_axis_known(count):
        while sum(t.shape[0] for t in tables) < count * own.shape[0]:
            sent = jnp.concatenate(tables, axis=0)
            n = len(tables) - 1
            tables.append(fetched(sent, "blk", 2**n))
        return tables
    for n, (shift, known) in enumerate(doublings(STEPS - 1)):
        by_shift = {}
        for array, shifts in zip(tables, known_places(STEPS - 1)):
            for at, shifted in enumerate(shifts):
                by_shift[shifted] = array[at * 2 * STEPS : (at + 1) * 2 * STEPS]
        sent = jnp.concatenate([by_shift[t] for t in range(-known, known + 1)], axis=0)
        for sign in (1, -1):
            tables.append(passed_along(sent, "blk", -sign * shift))
    return tables


def on_device(image, text, positive, logit_scale):
    rows, width = image.shape
    parts = lax.axis_size("rep")
    height = table_rows(parts)
    shape = jax.ShapeDtypeStruct
    texts, text_last = gathered_texts(text)
    direct, second, other = gathered_images(image)
    own_image, own_text = call(
        own_kernel, [shape((rows, width), BF16)] * 2, [VMEM] * 2, (image, text)
    )
    split = (parts - 1) * rows
    img_tiles, first, txt_first, row_first, col_first = call(
        functools.partial(first_kernel, parts),
        (
            shape((STEPS * rows, width), BF16),
            shape((STEPS * rows, split), F32),
            shape((split, width), BF16),
            shape((2 * STEPS + 1, rows), F32),
            shape((3 * (parts - 1), rows), F32),
        ),
        [SMEM] + [VMEM] * (6 + len(texts)),
        (logit_scale, positive, own_image, direct, second, other, own_text, *texts),
    )
    last, txt_last, row_stats, col_stats, row_pos = call(
        functools.partial(last_kernel, parts),
        (
            shape((STEPS * rows, rows), F32),
            shape((rows, width), BF16),
            shape((2 * STEPS, rows), F32),
            shape((height, rows), F32),
            shape((1, rows), F32),
        ),
        [SMEM] + [VMEM] * (4 + len(text_last)),
        (logit_scale, positive, img_tiles, row_first, col_first, *text_last),
        [pltpu.VMEM((2 * STEPS + 1, rows), F32), pltpu.VMEM((3, rows), F32)],
    )
    col_tables = [col_stats]
    for n, count in enumerate(slot_counts(parts)[1:]):
        sent = jnp.concatenate(col_tables, axis=0)[: count * height]
        col_tables.append(fetched(sent, "rep", 2**n))
    row_tables = known_row_tables(row_stats)
    n_kept = 2 if is_line(parts) else 1
    row_lse, col_lse, col_pos, weights, other, *narrow = call(
        functools.partial(weights_kernel, parts, len(row_tables)),
        (
            *[shape((1, rows), F32)] * 3,
            shape((STEPS * rows, parts * rows), BF16),
            *[shape((rows, width), BF16) for _ in range(1 + parts - n_kept)],
        ),
        [VMEM] * (6 + len(row_tables) + len(col_tables)),
        (
            positive,
            first,
            last,
            img_tiles,
            txt_first,
            txt_last,
            *row_tables,
            *col_tables,
        ),
        [pltpu.VMEM((sum(t.shape[0] for t in row_tables), rows), F32)],
    )
    swapped = neighbour_swapped(other)
    direct, second = call(
        passed_kernel,
        [shape((rows, width), BF16)] * 2,
        [VMEM] * 4,
        (weights, txt_first, txt_last, swapped),
    )
    own, *kept = call(
        rest_kernel,
        [shape((rows, width), F32) for _ in range(1 + n_kept)],
        [VMEM] * 4,
        (weights, img_tiles, txt_first, txt_last),
    )
    img_sums = [own, lax.ppermute(direct, "blk", direct_pairs()), passed_along(second, "blk", 2)]
    txt_sums = returned_texts(narrow, kept)
    grads = []
    for raw, (always, ends, others) in ((image, (img_sums, [], [])), (text, txt_sums)):
        sums = [*always, *ends, *others]
        grads.append(
            call(
                functools.partial(final_kernel, len(always), len(ends), parts),
                shape((rows, width), F32),
                [SMEM] + [VMEM] * (1 + len(sums)),
                (logit_scale, raw, *sums),
            )
        )
    row_loss = row_lse[0] - row_pos[0]
    col_loss = col_lse[0] - col_pos[0]
    return (row_loss, col_loss, *grads)


def solution(mesh):
    placed = (P(("blk", "rep"), None), P(("blk", "rep"), None), P("blk", "rep"), P())

    return jax.shard_map(
        on_device,
        mesh=mesh,
        in_specs=placed,
        out_specs=(
            P(("blk", "rep")),
            P(("blk", "rep")),
            P(("blk", "rep"), None),
            P(("blk", "rep"), None),
        ),
        check_vma=False,
    )
```
